256 devices in a mesh: ka: 8 (over y_hi, x), ga: 32 (over y_lo, z, core).
Axes of the slice: x: 4, y: 4 (y_hi: 2, y_lo: 2; y = y_hi * 2 + y_lo), z: 8, core: 2. Of those that a mesh axis runs over, the one named last changes fastest.
Arguments:
- orbitals: bfloat16 [16, 8, 2, 32, 1024], P('ka', None, None, 'ga'), may hold values from -6 to 6
- band_counts: int32 [16], replicated, may hold values from 1 to 8, as said below
- pair_slot: int32 [16, 16], replicated, may hold values from 0 to 15
- kernel: float32 [16, 32, 1024], P(None, None, 'ga'), may hold values from 0.2 to 8
Outputs:
- exchange_vectors: float32 [16, 8, 2, 32, 1024], P('ka', None, None, 'ga')
- exchange_matrix: float32 [16, 2, 8, 8], P('ka')
- exchange_energy: float32 [], replicated
The draws below stay inside these ranges and needn't reach their ends.
Inputs may be any that keep to these rules, and one draw needn't show every extreme that they name: The first band_counts[k] band slots of k-point k are the occupied ones; some k-point has all 8 slots occupied.
All inputs are finite; a program needn't handle non-finite values.
Results may differ from the reference program's by a relative error of at most 0.0003.
Values may be sent and summed in bfloat16 or wider, within the bound.
No kernel may reach another device: no remote copies, remote signals or barrier semaphores. Data moves between devices by JAX's collectives and lax.ppermute only.
A program may use at most 128 MiB of HBM per device.

```python
import math
import jax
import jax.numpy as jnp
from jax import lax

G = 32
K_DEV = 2
BANDS = 8
STEPS = 2
KPOINTS = 16
N_KA = 8


def draw_band_counts(key, part):
    first_key, second_key, third_key = jax.random.split(key, 3)
    partial_fill = jax.random.randint(first_key, (KPOINTS,), 1, BANDS // 2 + 1)
    full_mark = jax.random.randint(second_key, (KPOINTS,), 0, 4) == 0
    counts = jnp.where(full_mark, BANDS, partial_fill)
    chosen = jax.random.randint(third_key, (), 0, KPOINTS)
    positions = jnp.arange(KPOINTS)
    counts = jnp.where(positions == chosen, BANDS, counts)
    return counts.astype(jnp.int32)


def with_ends(array, own_key, low, top_value):
    longest = array.shape.index(max(array.shape))
    spots = []
    for shift in (0, 1):
        where = [jax.random.randint(jax.random.fold_in(own_key, axis), (), 0, length) for axis, length in enumerate(array.shape)]
        where[longest] = (where[longest] + shift) % array.shape[longest]
        spots.append(tuple(where))
    return array.at[spots[0]].set(low).at[spots[1]].set(top_value)


def level_of(stream_key, extent, cuts, least, high):
    def one(axis_at, parts):
        steps = jax.random.uniform(jax.random.fold_in(jax.random.fold_in(stream_key, 6), axis_at), (parts,), jnp.float32, least / len(cuts), high / len(cuts))
        return jnp.repeat(jnp.exp(steps), extent[axis_at] // parts).reshape((-1,) + (1,) * (len(extent) - axis_at - 1))

    factor_of = one(*cuts[0])
    for cut in cuts[1:]:
        factor_of = factor_of * one(*cut)
    return factor_of


def gaussian(own_key, dims, scale, bound, cuts=(), kind=jnp.bfloat16):
    values = jax.random.normal(own_key, dims, jnp.float32) * scale
    if len(cuts) > 0:
        values = level_of(own_key, dims, cuts, -0.22, 0.18) * values
    return jnp.clip(values, min=-bound, max=bound).astype(kind)


def setup_inputs(seed: int = 0) -> dict:
    keys = jax.random.split(jax.random.key(seed), 5)
    orbitals = gaussian(keys[0], (KPOINTS, BANDS, 2, G, G * G), 1.0, 6.0, ((0, 8), (3, 32)))
    band_counts = draw_band_counts(jax.random.fold_in(keys[4], 71), 0)
    pair_slot = with_ends(jax.random.randint(keys[2], (KPOINTS, KPOINTS), 0, KPOINTS), jax.random.fold_in(keys[2], 1), 0, KPOINTS - 1).astype(jnp.int32)
    kernel = jnp.clip(jnp.exp(math.log(8.0) - 3.6888794 * jax.random.uniform(keys[3], (KPOINTS, G, G * G), jnp.float32) ** level_of(keys[3], (KPOINTS, G, G * G), ((2, 32),), -0.2, 0.2)), 0.2, 8.0)
    return dict(orbitals=orbitals, band_counts=band_counts, pair_slot=pair_slot, kernel=kernel)


highest = lax.Precision.HIGHEST


def contract(first_field, second_field):
    return jnp.einsum("kar,kbr->kab", first_field, second_field, precision=highest)


def reference(orbitals, band_counts, pair_slot, kernel):
    kpoints = orbitals.shape[0]
    band_count = orbitals.shape[1]
    points = orbitals.shape[3]
    volume = points * points * points
    occupied = (jnp.arange(band_count, dtype=jnp.int32)[None, :] < band_counts[:, None]).astype(jnp.float32)
    real_part = orbitals[:, :, 0].astype(jnp.float32)
    imag_part = orbitals[:, :, 1].astype(jnp.float32)
    grid_shape = (kpoints, band_count, points, points, points)
    orbital_field = lax.complex(real_part, imag_part).reshape(grid_shape)
    spectra_kernel = kernel.reshape(kpoints, points, points, points)

    def one_kpoint(kpoint):
        own_group = kpoint // K_DEV
        own_field = orbital_field[kpoint]
        total_real = jnp.zeros((band_count, points, points, points), jnp.float32)
        total_imag = jnp.zeros((band_count, points, points, points), jnp.float32)
        for rotation in range(STEPS):
            anchor = (own_group - rotation) % N_KA
            window = (anchor * K_DEV + jnp.arange(K_DEV, dtype=jnp.int32)).astype(jnp.int32)
            partner = orbital_field[window] * occupied[window][:, :, None, None, None]
            density = jnp.conj(partner)[None] * own_field[:, None, None]
            spectra = jnp.fft.fftn(density, axes=(3, 4, 5))
            chosen = spectra_kernel[pair_slot[kpoint, window]]
            potential = jnp.fft.ifftn(spectra * chosen[None, :, None], axes=(3, 4, 5))
            product_field = jnp.sum(partner[None] * potential, axis=(1, 2))
            total_real = total_real + jnp.real(product_field)
            total_imag = total_imag + jnp.imag(product_field)
        prefactor = -1.0 / kpoints
        stacked = jnp.stack((total_real, total_imag), axis=1)
        return stacked.reshape(band_count, 2, points, points * points) * prefactor

    exchange_vectors = lax.map(one_kpoint, jnp.arange(kpoints, dtype=jnp.int32))
    flat_orbitals = orbitals.astype(jnp.float32).reshape(kpoints, band_count, 2, volume)
    flat_vectors = exchange_vectors.reshape(kpoints, band_count, 2, volume)
    matrix_real = (contract(flat_orbitals[:, :, 0], flat_vectors[:, :, 0]) + contract(flat_orbitals[:, :, 1], flat_vectors[:, :, 1])) / volume
    matrix_imag = (contract(flat_orbitals[:, :, 0], flat_vectors[:, :, 1]) - contract(flat_orbitals[:, :, 1], flat_vectors[:, :, 0])) / volume
    exchange_matrix = jnp.stack((matrix_real, matrix_imag), axis=1)
    exchange_energy = jnp.sum(occupied * jnp.diagonal(matrix_real, axis1=1, axis2=2)) / (2.0 * kpoints)
    return exchange_vectors, exchange_matrix, exchange_energy
```

```python
import numpy as np
import jax
import jax.numpy as jnp
from jax import lax
from jax.experimental import pallas as pl
from jax.experimental.pallas import tpu as pltpu
from jax.sharding import PartitionSpec as P

highest = lax.Precision.HIGHEST
f32 = jnp.float32
bf16 = jnp.bfloat16


def embed(matrix):
    return np.block([[matrix.real, -matrix.imag], [matrix.imag, matrix.real]])


def split(matrix):
    high = matrix.astype(np.float32).astype(bf16)
    low = (matrix - high.astype(np.float64)).astype(np.float32).astype(bf16)
    return high, low


def constants():
    rows = np.arange(128)
    x_at, yh_at = rows // 8, rows % 8
    jj_at, glo_at, gxh_at = rows // 64, rows // 8 % 8, rows % 8
    forward, inverse = [], []
    for parity in range(2):
        gx_at = 4 * gxh_at + 2 * jj_at + parity
        phase = gx_at[:, None] * x_at[None, :] / 32.0 + glo_at[:, None] * yh_at[None, :] / 8.0
        real = embed(np.exp(-2j * np.pi * phase))
        for held, matrix in ((forward, real), (inverse, real.T)):
            high, low = split(matrix)
            held.append(np.concatenate((high, low, high), axis=1))
    lanes = np.arange(128)
    first, last = lanes // 32, lanes % 32
    phase = first[:, None] * first[None, :] / 4.0 + last[:, None] * last[None, :] / 32.0
    real = embed(np.exp(-2j * np.pi * phase)).T
    right = []
    for matrix in (real, real.T):
        high, low = split(matrix)
        right.append(np.concatenate((high, low, high), axis=0))
    turn = 2.0 * np.pi * (glo_at[:, None] * first[None, :]) / 32.0
    twiddle = np.stack((np.cos(turn), np.sin(turn))).astype(np.float32)
    return np.stack(forward + inverse), np.stack(right), twiddle


def two_terms(value):
    high = value.astype(bf16)
    low = (value - high.astype(f32)).astype(bf16)
    return high, low


def exchange_kernel(
    scale, first_call, trips, received, partners, left, right, twiddle, held, total,
    own, screen,
):
    for a in range(2):
        own[a] = received[:, 4 + a].astype(f32)
    raw = received[:, 6].astype(f32)
    raw = (raw[:, :8] + raw[:, 8:]) * scale
    raw = raw.reshape(4, 64, 128)
    lane_group = lax.broadcasted_iota(jnp.int32, (64, 128), 1) // 32
    for j in range(4):
        placed = jnp.zeros((64, 128), f32)
        for i in range(4):
            shift = (i - j) % 4 * 32
            moved = pltpu.roll(raw[i], shift, 1) if shift else raw[i]
            placed = jnp.where(lane_group == i, moved, placed)
        screen[j % 2, (j // 2) * 64 : (j // 2) * 64 + 64] = placed
    if first_call:
        total[...] = jnp.zeros_like(total)
    else:
        total[...] = held[...]

    def one_partner(b, carry):
        other = partners[:, b].astype(f32)
        other_real, other_imag = other[:, :8], other[:, 8:]
        sums, gaps = [[], []], [[], []]
        for a in range(2):
            own_real, own_imag = own[a, :, :8], own[a, :, 8:]
            density = (
                own_real * other_real + own_imag * other_imag,
                own_imag * other_real - own_real * other_imag,
            )
            for part in range(2):
                low, high = density[part][:16], density[part][16:]
                sums[part].append((low + high).reshape(128, 128))
                gaps[part].append((low - high).reshape(128, 128))
        back = []
        for parity, parts in enumerate((sums, gaps)):
            stacked = jnp.concatenate(
                [jnp.concatenate(parts[part], axis=1) for part in range(2)], axis=0
            )
            high, low = two_terms(stacked)
            turned = jnp.dot(
                left[parity],
                jnp.concatenate((high, high, low), axis=0),
                preferred_element_type=f32,
            )
            cosine, sine = twiddle[0], twiddle[1]
            lines = []
            for a in range(2):
                real = turned[:128, a * 128 : a * 128 + 128]
                imag = turned[128:, a * 128 : a * 128 + 128]
                lines.append(
                    jnp.concatenate((real * cosine + imag * sine, imag * cosine - real * sine), axis=1)
                )
            high, low = two_terms(jnp.concatenate(lines, axis=0))
            spectra = jnp.dot(
                jnp.concatenate((high, high, low), axis=1), right[0], preferred_element_type=f32
            )
            factor = screen[parity]
            factor = jnp.concatenate((factor, factor), axis=1)
            factor = jnp.concatenate((factor, factor), axis=0)
            high, low = two_terms(spectra * factor)
            lines = jnp.dot(
                jnp.concatenate((high, high, low), axis=1), right[1], preferred_element_type=f32
            )
            reals, imags = [], []
            for a in range(2):
                real = lines[a * 128 : a * 128 + 128, :128]
                imag = lines[a * 128 : a * 128 + 128, 128:]
                reals.append(real * cosine - imag * sine)
                imags.append(imag * cosine + real * sine)
            stacked = jnp.concatenate(
                (jnp.concatenate(reals, axis=1), jnp.concatenate(imags, axis=1)), axis=0
            )
            high, low = two_terms(stacked)
            back.append(
                jnp.dot(
                    left[2 + parity],
                    jnp.concatenate((high, high, low), axis=0),
                    preferred_element_type=f32,
                )
            )
        even, odd = back
        for side in range(2):
            field = even + odd if side == 0 else even - odd
            rows = slice(side * 16, side * 16 + 16)
            b_real, b_imag = other_real[rows], other_imag[rows]
            for a in range(2):
                real = field[:128, a * 128 : a * 128 + 128].reshape(16, 8, 128)
                imag = field[128:, a * 128 : a * 128 + 128].reshape(16, 8, 128)
                total[rows, 2 * a] += b_real * real - b_imag * imag
                total[rows, 2 * a + 1] += b_real * imag + b_imag * real
        return carry

    lax.fori_loop(0, trips[0], one_partner, 0)


def exchange(scale, trips, received, partners, left, right, twiddle, held):
    first_call = held is None
    vmem = pl.BlockSpec(memory_space=pltpu.VMEM)
    operands = [trips, received, partners, left, right, twiddle]
    specs = [pl.BlockSpec(memory_space=pltpu.SMEM)] + [vmem] * 5

    if first_call:

        def body(trips, received, partners, left, right, twiddle, *rest):
            exchange_kernel(scale, True, trips, received, partners, left, right, twiddle, None, *rest)

    else:
        operands.append(held)
        specs.append(vmem)

        def body(*refs):
            exchange_kernel(scale, False, *refs)

    return pl.pallas_call(
        body,
        out_shape=jax.ShapeDtypeStruct((32, 4, 8, 128), f32),
        in_specs=specs,
        out_specs=vmem,
        scratch_shapes=[pltpu.VMEM((2, 32, 16, 128), f32), pltpu.VMEM((2, 128, 128), f32)],
        cost_estimate=pl.CostEstimate(
            flops=4 * 12 * 2 * 512 * 256 * 256, bytes_accessed=4 << 20, transcendentals=0
        ),
        name="exchange_first" if first_call else "exchange_second",
    )(*operands)


def contract(first_field, second_field):
    return jnp.einsum("kar,kbr->kab", first_field, second_field, precision=highest)


def over_copies(shard, axis):
    peers = lax.axis_size(axis)
    return lax.all_to_all(
        jnp.broadcast_to(shard[None], (peers, *shard.shape)), axis, 0, 0, tiled=True
    ).sum(axis=0)


def on_device(orbitals, band_counts, pair_slot, kernel):
    left, right, twiddle = (jnp.asarray(table) for table in constants())
    groups = lax.axis_size("ka")
    own_group = lax.axis_index("ka")
    member = lax.axis_index("ga")
    core = member % 2
    chip = member // 2
    partner_group = (own_group - 1) % groups
    volume = 32768.0

    pairs = [(source, (source + 1) % groups) for source in range(groups)]
    before = lax.ppermute(orbitals, "ka", pairs)
    window = jnp.concatenate(
        (own_group * 2 + jnp.arange(2), partner_group * 2 + jnp.arange(2))
    ).astype(jnp.int32)

    both = jnp.stack((orbitals, before)).reshape(4, 4, 2, 16, 128)
    partners = jnp.swapaxes(both, 1, 2)[:, None]
    partners = jnp.broadcast_to(partners, (4, 4, 2, 4, 16, 128))
    owns = orbitals.reshape(1, 4, 2, 2, 16, 128)
    owns = jnp.broadcast_to(owns, (4, 4, 2, 2, 16, 128))
    slots = pair_slot[own_group * 2 + jnp.arange(2)][:, window].T.reshape(8)
    chosen = kernel.reshape(16, 8, 128)[slots]
    chosen_high = lax.reduce_precision(chosen, 8, 7)
    chosen_low = chosen - chosen_high
    chosen = jnp.concatenate((chosen_high.astype(bf16), chosen_low.astype(bf16)), axis=1).reshape(4, 2, 1, 1, 1, 16, 128)
    chosen = jnp.broadcast_to(chosen, (4, 2, 2, 2, 1, 16, 128)).reshape(4, 4, 2, 1, 16, 128)
    packed = jnp.concatenate((partners, owns, chosen), axis=3).reshape(32, 7, 16, 128)
    received = lax.all_to_all(packed, "ga", 0, 0, tiled=True)
    swapped = lax.ppermute(received[:, :4], "ga", [(i, i ^ 1) for i in range(32)])

    count = band_counts[window[chip // 4]]
    own_trips = (count - core + 1) // 2
    swapped_trips = (count - (1 - core) + 1) // 2
    scale = -1.0 / (16.0 * volume)
    total = exchange(scale, own_trips.reshape(1), received, received, left, right, twiddle, None)
    total = exchange(scale, swapped_trips.reshape(1), received, swapped, left, right, twiddle, total)

    returned = lax.all_to_all(total, "ga", 0, 0, tiled=True)
    vectors = returned.reshape(4, 2, 8, 2, 1024).sum(axis=0)
    flat_orbitals = orbitals.astype(f32).reshape(2, 8, 2, 1024)
    matrix_real = (
        contract(flat_orbitals[:, :, 0], vectors[:, :, 0])
        + contract(flat_orbitals[:, :, 1], vectors[:, :, 1])
    ) / volume
    matrix_imag = (
        contract(flat_orbitals[:, :, 0], vectors[:, :, 1])
        - contract(flat_orbitals[:, :, 1], vectors[:, :, 0])
    ) / volume
    matrix = over_copies(jnp.stack((matrix_real, matrix_imag), axis=1), "ga")
    own_counts = lax.dynamic_slice_in_dim(band_counts, own_group * 2, 2)
    occupied = (jnp.arange(8)[None, :] < own_counts[:, None]).astype(f32)
    energy_part = jnp.sum(occupied * jnp.diagonal(matrix[:, 0], axis1=1, axis2=2)) / 32.0
    energy = over_copies(energy_part, "ka")
    return (vectors.reshape(2, 8, 2, 1, 1024), matrix, energy)


def solution(mesh):
    in_specs = (P("ka", None, None, "ga", None), P(), P(), P(None, None, "ga"))
    out_specs = (P("ka", None, None, "ga", None), P("ka", None, None, None), P())
    return jax.shard_map(
        on_device, mesh=mesh, in_specs=in_specs, out_specs=out_specs, check_vma=False
    )
```

```python
import numpy as np
import jax
import jax.numpy as jnp
from jax import lax
from jax.experimental import pallas as pl
from jax.experimental.pallas import tpu as pltpu
from jax.sharding import PartitionSpec as P

highest = lax.Precision.HIGHEST
f32 = jnp.float32
bf16 = jnp.bfloat16


def embed(matrix):
    return np.block([[matrix.real, -matrix.imag], [matrix.imag, matrix.real]])


def split(matrix):
    high = matrix.astype(np.float32).astype(bf16)
    low = (matrix - high.astype(np.float64)).astype(np.float32).astype(bf16)
    return high, low


def constants():
    rows = np.arange(128)
    x_at, yh_at = rows // 8, rows % 8
    jj_at, glo_at, gxh_at = rows // 64, rows // 8 % 8, rows % 8
    forward, inverse = [], []
    for parity in range(2):
        gx_at = 4 * gxh_at + 2 * jj_at + parity
        phase = gx_at[:, None] * x_at[None, :] / 32.0 + glo_at[:, None] * yh_at[None, :] / 8.0
        real = embed(np.exp(-2j * np.pi * phase))
        for held, matrix in ((forward, real), (inverse, real.T)):
            high, low = split(matrix)
            held.append(np.concatenate((high, low), axis=1))
    lanes = np.arange(128)
    first, last = lanes // 32, lanes % 32
    phase = first[:, None] * first[None, :] / 4.0 + last[:, None] * last[None, :] / 32.0
    real = embed(np.exp(-2j * np.pi * phase)).T
    right = []
    for matrix in (real, real.T):
        high, low = split(matrix)
        right.append(np.concatenate((high, low), axis=0))
    turn = 2.0 * np.pi * (glo_at[:, None] * first[None, :]) / 32.0
    twiddle = np.stack((np.cos(turn), np.sin(turn))).astype(np.float32)
    return np.stack(forward + inverse), np.stack(right), twiddle


def two_terms(value):
    high = value.astype(bf16)
    low = (value - high.astype(f32)).astype(bf16)
    return high, low


MIB = 1 << 20


def place():
    group = lax.axis_index("ka")
    member = lax.axis_index("ga")
    return group, member, member // 2, member % 2


def pack_kernel(pair_slot, orbitals, before, kernel, packed):
    group = lax.axis_index("ka")
    partner_group = lax.rem(group + 7, 8)
    for k2 in range(4):
        source = orbitals if k2 < 2 else before
        second = (group if k2 < 2 else partner_group) * 2 + k2 % 2
        for k in range(2):
            slot = pair_slot[group * 2 + k, second]
            block = kernel[slot]
            high = block.astype(bf16)
            low = (block - high.astype(f32)).astype(bf16)
            unit = jnp.concatenate((high, low), axis=0)
            for chip in range(2):
                for core in range(2):
                    packed[k2 * 8 + k * 4 + chip * 2 + core, 6] = unit
        for b in range(8):
            unit = source[k2 % 2 * 8 + b]
            for aset in range(4):
                packed[k2 * 8 + aset * 2 + b % 2, b // 2] = unit
        for a in range(16):
            packed[k2 * 8 + a // 2, 4 + a % 2] = orbitals[a]


def pack(pair_slot, orbitals, before, kernel):
    vmem = pl.BlockSpec(memory_space=pltpu.VMEM)
    return pl.pallas_call(
        pack_kernel,
        out_shape=jax.ShapeDtypeStruct((32, 7, 16, 128), bf16),
        in_specs=[pl.BlockSpec(memory_space=pltpu.SMEM), vmem, vmem, vmem],
        out_specs=vmem,
        compiler_params=pltpu.CompilerParams(vmem_limit_bytes=4 * MIB),
        name="pack",
    )(pair_slot, orbitals, before, kernel)


def screen_of(received, scale, screen):
    raw = received[:, 6].astype(f32)
    raw = (raw[:, :8] + raw[:, 8:]) * scale
    raw = raw.reshape(4, 64, 128)
    lane_group = lax.broadcasted_iota(jnp.int32, (64, 128), 1) // 32
    for j in range(4):
        placed = jnp.zeros((64, 128), f32)
        for i in range(4):
            shift = (i - j) % 4 * 32
            moved = pltpu.roll(raw[i], shift, 1) if shift else raw[i]
            placed = jnp.where(lane_group == i, moved, placed)
        screen[j % 2, (j // 2) * 64 : (j // 2) * 64 + 64] = placed


def thrice(table, axis):
    size = table.shape[axis] // 2
    return jnp.concatenate((table, lax.slice_in_dim(table, 0, size, axis=axis)), axis=axis)


def through(parts, parity, left, right, twiddle, screen):
    stacked = jnp.concatenate([jnp.concatenate(parts[part], axis=1) for part in range(2)], axis=0)
    high, low = two_terms(stacked)
    turned = jnp.dot(
        thrice(left[parity], 1), jnp.concatenate((high, high, low), axis=0), preferred_element_type=f32
    )
    cosine, sine = twiddle[0], twiddle[1]
    lines = []
    for a in range(2):
        real = turned[:128, a * 128 : a * 128 + 128]
        imag = turned[128:, a * 128 : a * 128 + 128]
        lines.append(
            jnp.concatenate((real * cosine + imag * sine, imag * cosine - real * sine), axis=1)
        )
    high, low = two_terms(jnp.concatenate(lines, axis=0))
    spectra = jnp.dot(
        jnp.concatenate((high, high, low), axis=1), thrice(right[0], 0), preferred_element_type=f32
    )
    factor = screen[parity]
    factor = jnp.concatenate((factor, factor), axis=1)
    factor = jnp.concatenate((factor, factor), axis=0)
    high, low = two_terms(spectra * factor)
    lines = jnp.dot(
        jnp.concatenate((high, high, low), axis=1), thrice(right[1], 0), preferred_element_type=f32
    )
    reals, imags = [], []
    for a in range(2):
        real = lines[a * 128 : a * 128 + 128, :128]
        imag = lines[a * 128 : a * 128 + 128, 128:]
        reals.append(real * cosine - imag * sine)
        imags.append(imag * cosine + real * sine)
    stacked = jnp.concatenate(
        (jnp.concatenate(reals, axis=1), jnp.concatenate(imags, axis=1)), axis=0
    )
    high, low = two_terms(stacked)
    return jnp.dot(
        thrice(left[2 + parity], 1), jnp.concatenate((high, high, low), axis=0), preferred_element_type=f32
    )


def exchange_kernel(
    scale, second_call, counts, received, partners, left, right, twiddle, held, total, energy,
    own, screen,
):
    group, member, chip, core = place()
    k2 = chip // 4
    k2_at = lax.rem(group + 8 - k2 // 2, 8) * 2 + k2 % 2
    parity_of_b = 1 - core if second_call else core
    trips = (counts[k2_at] - parity_of_b + 1) // 2
    for a in range(2):
        own[a] = received[:, 4 + a].astype(f32)
    screen_of(received, scale, screen)
    if second_call:
        total[...] = held[...]
    else:
        total[...] = jnp.zeros_like(total)

    def turn(step, carry):
        others, backs = [], []
        for half in range(UNROLL):
            b = step * UNROLL + half
            other = partners[:, b].astype(f32)
            if half:
                other = other * jnp.where(b < trips, 1.0, 0.0).astype(f32)
            other_real, other_imag = other[:, :8], other[:, 8:]
            sums, gaps = [[], []], [[], []]
            for a in range(2):
                own_real, own_imag = own[a, :, :8], own[a, :, 8:]
                density = (
                    own_real * other_real + own_imag * other_imag,
                    own_imag * other_real - own_real * other_imag,
                )
                for part in range(2):
                    low, high = density[part][:16], density[part][16:]
                    sums[part].append((low + high).reshape(128, 128))
                    gaps[part].append((low - high).reshape(128, 128))
            others.append((other_real, other_imag))
            backs.append(
                [
                    through(parts, parity, left, right, twiddle, screen)
                    for parity, parts in enumerate((sums, gaps))
                ]
            )
        for side in range(2):
            rows = slice(side * 16, side * 16 + 16)
            for a in range(2):
                add_real, add_imag = 0.0, 0.0
                for (even, odd), (other_real, other_imag) in zip(backs, others):
                    field = even + odd if side == 0 else even - odd
                    b_real, b_imag = other_real[rows], other_imag[rows]
                    real = field[:128, a * 128 : a * 128 + 128].reshape(16, 8, 128)
                    imag = field[128:, a * 128 : a * 128 + 128].reshape(16, 8, 128)
                    add_real += b_real * real - b_imag * imag
                    add_imag += b_real * imag + b_imag * real
                total[rows, 2 * a] += add_real
                total[rows, 2 * a + 1] += add_imag
        return carry

    lax.fori_loop(0, (trips + UNROLL - 1) // UNROLL, turn, 0)

    if second_call:
        energy_sum = jnp.zeros((8, 128), f32)
        for a in range(2):
            flat = lax.rem(chip, 4) * 4 + core * 2 + a
            occupied = jnp.where(lax.rem(flat, 8) < counts[group * 2 + flat // 8], 1.0, 0.0)
            both = own[a, :, :8] * total[:, 2 * a] + own[a, :, 8:] * total[:, 2 * a + 1]
            energy_sum += jnp.sum(both, axis=0) * occupied.astype(f32)
        energy[...] = jnp.full((8, 128), jnp.sum(energy_sum) * (1.0 / (32.0 * 32768.0)), f32)


UNROLL = 2


def exchange(scale, counts, received, partners, left, right, twiddle, held):
    second_call = held is not None
    vmem = pl.BlockSpec(memory_space=pltpu.VMEM)
    operands = [counts, received, partners, left, right, twiddle]
    specs = [pl.BlockSpec(memory_space=pltpu.SMEM)] + [vmem] * 5
    field = jax.ShapeDtypeStruct((32, 4, 8, 128), f32)
    aliases = {}
    if second_call:
        operands.append(held)
        specs.append(vmem)
        aliases = {6: 0}
        out_shape, out_specs = (field, jax.ShapeDtypeStruct((8, 128), f32)), (vmem, vmem)

        def body(*refs):
            exchange_kernel(scale, True, *refs)

    else:
        out_shape, out_specs = field, vmem

        def body(counts, received, partners, left, right, twiddle, total, own, screen):
            exchange_kernel(
                scale, False, counts, received, partners, left, right, twiddle, None, total, None,
                own, screen,
            )

    return pl.pallas_call(
        body,
        out_shape=out_shape,
        in_specs=specs,
        out_specs=out_specs,
        scratch_shapes=[pltpu.VMEM((2, 32, 16, 128), f32), pltpu.VMEM((2, 128, 128), f32)],
        input_output_aliases=aliases,
        compiler_params=pltpu.CompilerParams(vmem_limit_bytes=24 * MIB),
        cost_estimate=pl.CostEstimate(
            flops=4 * 12 * 2 * 512 * 256 * 256, bytes_accessed=4 << 20, transcendentals=0
        ),
        name="exchange_second" if second_call else "exchange_first",
    )(*operands)


def finish_kernel(returned, orbitals, energies, vectors, message):
    fields = returned[0] + returned[1] + returned[2] + returned[3]
    vectors[...] = fields
    fields = fields.reshape(16, 2, 8, 128)
    sums = []
    for k in range(2):
        own = orbitals[k * 8 : k * 8 + 8].astype(f32)
        own_real, own_imag = own[:, None, :8], own[:, None, 8:]
        real = fields[None, k * 8 : k * 8 + 8, 0]
        imag = fields[None, k * 8 : k * 8 + 8, 1]
        for product in (own_real * real + own_imag * imag, own_real * imag - own_imag * real):
            sums.append(jnp.sum(product, axis=2).reshape(64, 128))
    sums = jnp.concatenate(sums, axis=0)
    flat = lax.dot_general(
        jnp.full((8, 128), 1.0 / 32768.0, f32), sums, (((1,), (1,)), ((), ())),
        precision=highest, preferred_element_type=f32,
    )
    total = energies[:1]
    rows = jnp.concatenate((flat[:1, :128], flat[:1, 128:], total, total), axis=0)
    message[...] = jnp.broadcast_to(rows[None], (32, 4, 128))


def finish(returned, orbitals, energies):
    vmem = pl.BlockSpec(memory_space=pltpu.VMEM)
    return pl.pallas_call(
        finish_kernel,
        out_shape=(
            jax.ShapeDtypeStruct((32, 8, 128), f32),
            jax.ShapeDtypeStruct((32, 4, 128), f32),
        ),
        in_specs=[vmem] * 3,
        out_specs=(vmem, vmem),
        compiler_params=pltpu.CompilerParams(vmem_limit_bytes=8 * MIB),
        name="finish",
    )(returned, orbitals, energies)


def on_device(orbitals, band_counts, pair_slot, kernel):
    left, right, twiddle = (jnp.asarray(table) for table in constants())
    groups = lax.axis_size("ka")
    scale = -1.0 / (16.0 * 32768.0)

    orbitals = orbitals.reshape(16, 16, 128)
    before = lax.ppermute(orbitals, "ka", [(i, (i + 1) % groups) for i in range(groups)])
    packed = pack(pair_slot, orbitals, before, kernel.reshape(16, 8, 128))
    received = lax.all_to_all(packed, "ga", 0, 0, tiled=True)
    swapped = lax.ppermute(received[:, :4], "ga", [(i, i ^ 1) for i in range(32)])
    total = exchange(scale, band_counts, received, received, left, right, twiddle, None)
    total, energy = exchange(scale, band_counts, received, swapped, left, right, twiddle, total)

    returned = lax.all_to_all(total, "ga", 0, 0, tiled=True)
    for step in (1, 2, 4):
        energy = energy + lax.ppermute(energy, "ka", [(i, i ^ step) for i in range(groups)])
    vectors, message = finish(returned.reshape(4, 32, 8, 128), orbitals, energy)
    sums = lax.all_to_all(message, "ga", 0, 0, tiled=True).sum(axis=0)
    return (
        vectors.reshape(2, 8, 2, 1, 1024),
        sums[:2].reshape(2, 2, 8, 8),
        sums[2, 0],
    )


def solution(mesh):
    in_specs = (P("ka", None, None, "ga", None), P(), P(), P(None, None, "ga"))
    out_specs = (P("ka", None, None, "ga", None), P("ka", None, None, None), P())
    return jax.shard_map(
        on_device, mesh=mesh, in_specs=in_specs, out_specs=out_specs, check_vma=False
    )
```

```python
import functools

import numpy as np
import jax
import jax.numpy as jnp
from jax import lax
from jax.experimental import pallas as pl
from jax.experimental.pallas import tpu as pltpu
from jax.sharding import PartitionSpec as P

highest = lax.Precision.HIGHEST
f32 = jnp.float32
bf16 = jnp.bfloat16


def embed(matrix):
    return np.block([[matrix.real, -matrix.imag], [matrix.imag, matrix.real]])


def split(matrix):
    high = matrix.astype(np.float32).astype(bf16)
    low = (matrix - high.astype(np.float64)).astype(np.float32).astype(bf16)
    return high, low


def constants():
    rows = np.arange(128)
    x_at, yh_at = rows // 8, rows % 8
    jj_at, glo_at, gxh_at = rows // 64, rows // 8 % 8, rows % 8
    forward, inverse = [], []
    for parity in range(2):
        gx_at = 4 * gxh_at + 2 * jj_at + parity
        phase = gx_at[:, None] * x_at[None, :] / 32.0 + glo_at[:, None] * yh_at[None, :] / 8.0
        real = embed(np.exp(-2j * np.pi * phase))
        for held, matrix in ((forward, real), (inverse, real.T)):
            high, low = split(matrix)
            held.append(np.concatenate((high, low), axis=1))
    lanes = np.arange(128)
    first, last = lanes // 32, lanes % 32
    phase = first[:, None] * first[None, :] / 4.0 + last[:, None] * last[None, :] / 32.0
    real = embed(np.exp(-2j * np.pi * phase)).T
    right = []
    for matrix in (real, real.T):
        high, low = split(matrix)
        right.append(np.concatenate((high, low), axis=0))
    turn = 2.0 * np.pi * (glo_at[:, None] * first[None, :]) / 32.0
    twiddle = np.stack((np.cos(turn), np.sin(turn))).astype(np.float32)
    return np.stack(forward + inverse), np.stack(right), twiddle


def two_terms(value):
    high = value.astype(bf16)
    low = (value - high.astype(f32)).astype(bf16)
    return high, low


MIB = 1 << 20


def place():
    member = lax.axis_index("ga")
    return lax.axis_index("ka"), member // 16, member // 4 % 4, member // 2 % 2, member % 2


def pack_kernel(pair_slot, orbitals, before, kernel, packed):
    group = lax.axis_index("ka")
    partner_group = lax.rem(group + 7, 8)
    for k2 in range(4):
        source = orbitals if k2 < 2 else before
        second = (group if k2 < 2 else partner_group) * 2 + k2 % 2
        for k in range(2):
            slot = pair_slot[group * 2 + k, second]
            block = kernel[slot]
            high = block.astype(bf16)
            low = (block - high.astype(f32)).astype(bf16)
            unit = jnp.concatenate((high, low), axis=0)
            for quarter in range(4):
                to = quarter // 2 * 16 + k2 * 4 + k * 2 + quarter % 2
                for j in range(2):
                    packed[to, j] = source[k2 % 2 * 8 + quarter * 2 + j]
                    packed[to, 2 + j] = orbitals[k * 8 + quarter * 2 + j]
                packed[to, 4] = unit


def pack(pair_slot, orbitals, before, kernel):
    vmem = pl.BlockSpec(memory_space=pltpu.VMEM)
    return pl.pallas_call(
        pack_kernel,
        out_shape=jax.ShapeDtypeStruct((32, 5, 16, 128), bf16),
        in_specs=[pl.BlockSpec(memory_space=pltpu.SMEM), vmem, vmem, vmem],
        out_specs=vmem,
        compiler_params=pltpu.CompilerParams(vmem_limit_bytes=4 * MIB),
        name="pack",
    )(pair_slot, orbitals, before, kernel)


def screen_of(received, scale, screen):
    raw = received[:, 4].astype(f32)
    raw = (raw[:, :8] + raw[:, 8:]) * scale
    raw = raw.reshape(4, 64, 128)
    lane_group = lax.broadcasted_iota(jnp.int32, (64, 128), 1) // 32
    for j in range(4):
        placed = jnp.zeros((64, 128), f32)
        for i in range(4):
            shift = (i - j) % 4 * 32
            moved = pltpu.roll(raw[i], shift, 1) if shift else raw[i]
            placed = jnp.where(lane_group == i, moved, placed)
        screen[j % 2, (j // 2) * 64 : (j // 2) * 64 + 64] = placed


def thrice(table, axis):
    size = table.shape[axis] // 2
    return jnp.concatenate((table, lax.slice_in_dim(table, 0, size, axis=axis)), axis=axis)


def enter(parts, table):
    stacked = jnp.concatenate([jnp.concatenate(parts[part], axis=1) for part in range(2)], axis=0)
    high, low = two_terms(stacked)
    return jnp.dot(
        thrice(table, 1), jnp.concatenate((high, high, low), axis=0), preferred_element_type=f32
    )


def across(turned, table, cosine, sine):
    lines = []
    for a in range(2):
        real = turned[:128, a * 128 : a * 128 + 128]
        imag = turned[128:, a * 128 : a * 128 + 128]
        lines.append(
            jnp.concatenate((real * cosine + imag * sine, imag * cosine - real * sine), axis=1)
        )
    high, low = two_terms(jnp.concatenate(lines, axis=0))
    return jnp.dot(
        jnp.concatenate((high, high, low), axis=1), thrice(table, 0), preferred_element_type=f32
    )


def screened(spectra, factor, table):
    factor = jnp.concatenate((factor, factor), axis=1)
    factor = jnp.concatenate((factor, factor), axis=0)
    high, low = two_terms(spectra * factor)
    return jnp.dot(
        jnp.concatenate((high, high, low), axis=1), thrice(table, 0), preferred_element_type=f32
    )


def leave(lines, table, cosine, sine):
    reals, imags = [], []
    for a in range(2):
        real = lines[a * 128 : a * 128 + 128, :128]
        imag = lines[a * 128 : a * 128 + 128, 128:]
        reals.append(real * cosine - imag * sine)
        imags.append(imag * cosine + real * sine)
    stacked = jnp.concatenate(
        (jnp.concatenate(reals, axis=1), jnp.concatenate(imags, axis=1)), axis=0
    )
    high, low = two_terms(stacked)
    return jnp.dot(
        thrice(table, 1), jnp.concatenate((high, high, low), axis=0), preferred_element_type=f32
    )


def exchange_kernel(scale, call, counts, received, partners, left, right, twiddle, *rest):
    if call == 0:
        total, screen = rest
        screen_of(received, scale, screen)
        held = None
    elif call < 3:
        screen, held, total = rest
    else:
        screen, held, total, energy = rest
    group, y_at, k2, k, core = place()
    k2_at = lax.rem(group + 8 - k2 // 2, 8) * 2 + k2 % 2
    quarter = (1 - y_at if call >= 2 else y_at) * 2 + (1 - core if call % 2 else core)
    occupied_here = counts[k2_at] - 2 * quarter

    @pl.when(occupied_here > 0)
    def _():
        second_kept = jnp.where(occupied_here > 1, 1.0, 0.0).astype(f32)
        others, chains = [], []
        for half in range(2):
            other = partners[:, half].astype(f32)
            if half:
                other = other * second_kept
            other_real, other_imag = other[:, :8], other[:, 8:]
            sums, gaps = [[], []], [[], []]
            for a in range(2):
                own = received[:, 2 + a].astype(f32)
                own_real, own_imag = own[:, :8], own[:, 8:]
                density = (
                    own_real * other_real + own_imag * other_imag,
                    own_imag * other_real - own_real * other_imag,
                )
                for part in range(2):
                    low, high = density[part][:16], density[part][16:]
                    sums[part].append((low + high).reshape(128, 128))
                    gaps[part].append((low - high).reshape(128, 128))
            others.append((other_real, other_imag))
            chains += [(0, sums), (1, gaps)]
        cosine, sine = twiddle[0], twiddle[1]
        values = [enter(parts, left[parity]) for parity, parts in chains]
        values = [across(value, right[0], cosine, sine) for value in values]
        values = [
            screened(value, screen[parity], right[1])
            for value, (parity, parts) in zip(values, chains)
        ]
        values = [
            leave(value, left[2 + parity], cosine, sine)
            for value, (parity, parts) in zip(values, chains)
        ]
        backs = [values[2 * half : 2 * half + 2] for half in range(2)]
        for side in range(2):
            rows = slice(side * 16, side * 16 + 16)
            for a in range(2):
                add_real, add_imag = 0.0, 0.0
                if held is not None:
                    add_real, add_imag = held[rows, 2 * a], held[rows, 2 * a + 1]
                for (even, odd), (other_real, other_imag) in zip(backs, others):
                    field = even + odd if side == 0 else even - odd
                    b_real, b_imag = other_real[rows], other_imag[rows]
                    real = field[:128, a * 128 : a * 128 + 128].reshape(16, 8, 128)
                    imag = field[128:, a * 128 : a * 128 + 128].reshape(16, 8, 128)
                    add_real += b_real * real - b_imag * imag
                    add_imag += b_real * imag + b_imag * real
                total[rows, 2 * a] = add_real
                total[rows, 2 * a + 1] = add_imag

    @pl.when(occupied_here <= 0)
    def _():
        total[...] = jnp.zeros_like(total) if held is None else held[...]

    if call == 3:
        energy_sum = jnp.zeros((8, 128), f32)
        for a in range(2):
            band = y_at * 4 + core * 2 + a
            occupied = jnp.where(band < counts[group * 2 + k], 1.0, 0.0).astype(f32)
            own = received[:, 2 + a].astype(f32)
            both = own[:, :8] * total[:, 2 * a] + own[:, 8:] * total[:, 2 * a + 1]
            energy_sum += jnp.sum(both, axis=0) * occupied
        energy[...] = jnp.full((8, 128), jnp.sum(energy_sum) * (1.0 / (32.0 * 32768.0)), f32)


def exchange(scale, call, counts, received, partners, left, right, twiddle, *carried):
    vmem = pl.BlockSpec(memory_space=pltpu.VMEM)
    operands = (counts, received, partners, left, right, twiddle, *carried)
    shapes = [jax.ShapeDtypeStruct((32, 4, 8, 128), f32)]
    if call == 0:
        shapes.append(jax.ShapeDtypeStruct((2, 128, 128), f32))
    if call == 3:
        shapes.append(jax.ShapeDtypeStruct((8, 128), f32))
    return pl.pallas_call(
        functools.partial(exchange_kernel, scale, call),
        out_shape=tuple(shapes),
        in_specs=[pl.BlockSpec(memory_space=pltpu.SMEM)] + [vmem] * (len(operands) - 1),
        out_specs=(vmem,) * len(shapes),
        compiler_params=pltpu.CompilerParams(vmem_limit_bytes=24 * MIB),
        cost_estimate=pl.CostEstimate(
            flops=2 * 12 * 2 * 512 * 256 * 256, bytes_accessed=4 << 20, transcendentals=0
        ),
        name=("exchange_0", "exchange_1", "exchange_2", "exchange_3")[call],
    )(*operands)


def finish_kernel(returned, orbitals, energies, vectors, message):
    fields = []
    for k in range(2):
        for y_at in range(2):
            fields.append(sum(returned[y_at, k2, k] for k2 in range(4)))
    fields = jnp.concatenate(fields, axis=0)
    vectors[...] = fields
    fields = fields.reshape(16, 2, 8, 128)
    sums = []
    for k in range(2):
        own = orbitals[k * 8 : k * 8 + 8].astype(f32)
        own_real, own_imag = own[:, None, :8], own[:, None, 8:]
        real = fields[None, k * 8 : k * 8 + 8, 0]
        imag = fields[None, k * 8 : k * 8 + 8, 1]
        for product in (own_real * real + own_imag * imag, own_real * imag - own_imag * real):
            sums.append(jnp.sum(product, axis=2).reshape(64, 128))
    sums = jnp.concatenate(sums, axis=0)
    flat = lax.dot_general(
        jnp.full((8, 128), 1.0 / 32768.0, f32), sums, (((1,), (1,)), ((), ())),
        precision=highest, preferred_element_type=f32,
    )
    total = energies[:1]
    rows = jnp.concatenate((flat[:1, :128], flat[:1, 128:], total, total), axis=0)
    message[...] = jnp.broadcast_to(rows[None], (32, 4, 128))


def finish(returned, orbitals, energies):
    vmem = pl.BlockSpec(memory_space=pltpu.VMEM)
    return pl.pallas_call(
        finish_kernel,
        out_shape=(
            jax.ShapeDtypeStruct((32, 8, 128), f32),
            jax.ShapeDtypeStruct((32, 4, 128), f32),
        ),
        in_specs=[vmem] * 3,
        out_specs=(vmem, vmem),
        compiler_params=pltpu.CompilerParams(vmem_limit_bytes=8 * MIB),
        name="finish",
    )(returned, orbitals, energies)


def close_kernel(messages, matrix, energy):
    total = jnp.sum(messages[...], axis=0)
    lane = lax.broadcasted_iota(jnp.int32, (32, 128), 1)
    row = lax.broadcasted_iota(jnp.int32, (32, 128), 0)
    spread = jnp.concatenate(
        [jnp.broadcast_to(total[k : k + 1], (16, 128)) for k in range(2)], axis=0
    )
    spread = jnp.where(lane // 8 == row % 16, spread, 0.0)
    gather = jnp.where(
        lax.broadcasted_iota(jnp.int32, (128, 128), 0) % 8
        == lax.broadcasted_iota(jnp.int32, (128, 128), 1),
        1.0,
        0.0,
    )
    spread = jnp.dot(spread, gather, precision=highest, preferred_element_type=f32)
    for k in range(2):
        for part in range(2):
            first = k * 16 + part * 8
            matrix[k, part] = spread[first : first + 8, :8]
    energy[...] = total[2:3, :1]


def close(messages):
    vmem = pl.BlockSpec(memory_space=pltpu.VMEM)
    return pl.pallas_call(
        close_kernel,
        out_shape=(jax.ShapeDtypeStruct((2, 2, 8, 8), f32), jax.ShapeDtypeStruct((1, 1), f32)),
        in_specs=[vmem],
        out_specs=(vmem, vmem),
        compiler_params=pltpu.CompilerParams(vmem_limit_bytes=4 * MIB),
        name="close",
    )(messages)


def on_device(orbitals, band_counts, pair_slot, kernel):
    left, right, twiddle = (jnp.asarray(table) for table in constants())
    groups = lax.axis_size("ka")
    scale = -1.0 / (16.0 * 32768.0)

    orbitals = orbitals.reshape(16, 16, 128)
    before = lax.ppermute(orbitals, "ka", [(i, (i + 1) % groups) for i in range(groups)])
    packed = pack(pair_slot, orbitals, before, kernel.reshape(16, 8, 128))
    received = lax.all_to_all(packed, "ga", 0, 0, tiled=True)

    def shown(value, bit):
        return lax.ppermute(value, "ga", [(i, i ^ bit) for i in range(32)])

    mine = received[:, :2]
    next_y = shown(mine, 16)
    next_core = shown(mine, 1)
    tables = (left, right, twiddle)
    total, screen = exchange(scale, 0, band_counts, received, received, *tables)
    (total,) = exchange(scale, 1, band_counts, received, next_core, *tables, screen, total)
    next_y, total = lax.optimization_barrier((next_y, total))
    next_both = shown(next_y, 1)
    (total,) = exchange(scale, 2, band_counts, received, next_y, *tables, screen, total)
    total, energy = exchange(scale, 3, band_counts, received, next_both, *tables, screen, total)

    returned = lax.all_to_all(total, "ga", 0, 0, tiled=True)
    for bit in (1, 2, 4):
        energy = energy + lax.ppermute(energy, "ka", [(i, i ^ bit) for i in range(groups)])
    vectors, message = finish(returned.reshape(2, 4, 2, 8, 8, 128), orbitals, energy)
    matrix, energy = close(lax.all_to_all(message, "ga", 0, 0, tiled=True))
    return (vectors.reshape(2, 8, 2, 1, 1024), matrix, energy[0, 0])


def solution(mesh):
    in_specs = (P("ka", None, None, "ga", None), P(), P(), P(None, None, "ga"))
    out_specs = (P("ka", None, None, "ga", None), P("ka", None, None, None), P())
    return jax.shard_map(
        on_device, mesh=mesh, in_specs=in_specs, out_specs=out_specs, check_vma=False
    )
```

```python
import functools

import numpy as np
import jax
import jax.numpy as jnp
from jax import lax
from jax.experimental import pallas as pl
from jax.experimental.pallas import tpu as pltpu
from jax.sharding import PartitionSpec as P

highest = lax.Precision.HIGHEST
f32 = jnp.float32
bf16 = jnp.bfloat16


def embed(matrix):
    return np.block([[matrix.real, -matrix.imag], [matrix.imag, matrix.real]])


def split(matrix):
    high = matrix.astype(np.float32).astype(bf16)
    low = (matrix - high.astype(np.float64)).astype(np.float32).astype(bf16)
    return high, low


def constants():
    rows = np.arange(128)
    x_at, yh_at = rows // 8, rows % 8
    jj_at, glo_at, gxh_at = rows // 64, rows // 8 % 8, rows % 8
    forward, inverse = [], []
    for parity in range(2):
        gx_at = 4 * gxh_at + 2 * jj_at + parity
        phase = gx_at[:, None] * x_at[None, :] / 32.0 + glo_at[:, None] * yh_at[None, :] / 8.0
        real = embed(np.exp(-2j * np.pi * phase))
        for held, matrix in ((forward, real), (inverse, real.T)):
            high, low = split(matrix)
            held.append(np.concatenate((high, low), axis=1))
    lanes = np.arange(128)
    first, last = lanes // 32, lanes % 32
    phase = first[:, None] * first[None, :] / 4.0 + last[:, None] * last[None, :] / 32.0
    real = embed(np.exp(-2j * np.pi * phase)).T
    right = []
    for matrix in (real, real.T):
        high, low = split(matrix)
        right.append(np.concatenate((high, low), axis=0))
    turn = 2.0 * np.pi * (glo_at[:, None] * first[None, :]) / 32.0
    twiddle = np.stack((np.cos(turn), np.sin(turn))).astype(np.float32)
    return np.stack(forward + inverse), np.stack(right), twiddle


def two_terms(value):
    high = value.astype(bf16)
    low = (value - high.astype(f32)).astype(bf16)
    return high, low


MIB = 1 << 20


def place():
    member = lax.axis_index("ga")
    return lax.axis_index("ka"), member // 16, member // 4 % 4, member // 2 % 2, member % 2


def y_band(y_at, core):
    return 4 * y_at + core


def z_band(y_at, k, core):
    return 2 + 4 * ((y_at + k) % 2) + core


def choose_kernel(pair_slot, kernel, chosen):
    group = lax.axis_index("ka")
    partner_group = lax.rem(group + 7, 8)
    for k2 in range(4):
        second = (group if k2 < 2 else partner_group) * 2 + k2 % 2
        for k in range(2):
            block = kernel[pair_slot[group * 2 + k, second]]
            high, low = two_terms(block)
            for core in range(2):
                rows = slice(core * 4, core * 4 + 4)
                chosen[k2 * 2 + k, core] = jnp.concatenate((high[rows], low[rows]), axis=0)


def choose(pair_slot, kernel):
    vmem = pl.BlockSpec(memory_space=pltpu.VMEM)
    return pl.pallas_call(
        choose_kernel,
        out_shape=jax.ShapeDtypeStruct((8, 2, 8, 128), bf16),
        in_specs=[pl.BlockSpec(memory_space=pltpu.SMEM), vmem],
        out_specs=vmem,
        compiler_params=pltpu.CompilerParams(vmem_limit_bytes=4 * MIB),
        name="choose",
    )(pair_slot, kernel)


KERNEL_ROWS = slice(0, 8)
BAND_ROWS = (slice(8, 24), slice(24, 40))
OWN_ROWS = (slice(40, 56), slice(56, 72))


def pack_kernel(orbitals, before, chosen, packed):
    for k2 in range(4):
        source = orbitals if k2 < 2 else before
        for k in range(2):
            for quarter in range(4):
                y_at, core = quarter // 2, quarter % 2
                to = y_at * 16 + k2 * 4 + k * 2 + core
                packed[to, KERNEL_ROWS] = chosen[k2 * 2 + k, core]
                packed[to, BAND_ROWS[0]] = source[k2 % 2 * 8 + y_band(y_at, core)]
                packed[to, BAND_ROWS[1]] = source[k2 % 2 * 8 + z_band(y_at, k, core)]
                for j in range(2):
                    packed[to, OWN_ROWS[j]] = orbitals[k * 8 + quarter * 2 + j]


def pack(orbitals, before, chosen):
    vmem = pl.BlockSpec(memory_space=pltpu.VMEM)
    return pl.pallas_call(
        pack_kernel,
        out_shape=jax.ShapeDtypeStruct((32, 72, 128), bf16),
        in_specs=[vmem, vmem, vmem],
        out_specs=vmem,
        compiler_params=pltpu.CompilerParams(vmem_limit_bytes=4 * MIB),
        name="pack",
    )(orbitals, before, chosen)


def screen_of(received, other, core, scale, screen):
    halves = []
    for half in (received, other):
        half = half[:, KERNEL_ROWS].astype(f32)
        halves.append(((half + pltpu.roll(half, 4, 1)) * scale).reshape(256, 128))
    row = lax.broadcasted_iota(jnp.int32, (256, 128), 0) % 8
    raw = jnp.where(row // 4 == core, halves[0], halves[1]).reshape(4, 64, 128)
    lane_group = lax.broadcasted_iota(jnp.int32, (64, 128), 1) // 32
    for j in range(4):
        placed = jnp.zeros((64, 128), f32)
        for i in range(4):
            shift = (i - j) % 4 * 32
            moved = pltpu.roll(raw[i], shift, 1) if shift else raw[i]
            placed = jnp.where(lane_group == i, moved, placed)
        screen[j % 2, (j // 2) * 64 : (j // 2) * 64 + 64] = placed


def thrice(table, axis):
    size = table.shape[axis] // 2
    return jnp.concatenate((table, lax.slice_in_dim(table, 0, size, axis=axis)), axis=axis)


def enter(parts, table):
    stacked = jnp.concatenate([jnp.concatenate(parts[part], axis=1) for part in range(2)], axis=0)
    high, low = two_terms(stacked)
    return jnp.dot(
        thrice(table, 1), jnp.concatenate((high, high, low), axis=0), preferred_element_type=f32
    )


def across(turned, table, cosine, sine):
    lines = []
    for a in range(2):
        real = turned[:128, a * 128 : a * 128 + 128]
        imag = turned[128:, a * 128 : a * 128 + 128]
        lines.append(
            jnp.concatenate((real * cosine + imag * sine, imag * cosine - real * sine), axis=1)
        )
    high, low = two_terms(jnp.concatenate(lines, axis=0))
    return jnp.dot(
        jnp.concatenate((high, high, low), axis=1), thrice(table, 0), preferred_element_type=f32
    )


def screened(spectra, factor, table):
    factor = jnp.concatenate((factor, factor), axis=1)
    factor = jnp.concatenate((factor, factor), axis=0)
    high, low = two_terms(spectra * factor)
    return jnp.dot(
        jnp.concatenate((high, high, low), axis=1), thrice(table, 0), preferred_element_type=f32
    )


def leave(lines, table, cosine, sine):
    reals, imags = [], []
    for a in range(2):
        real = lines[a * 128 : a * 128 + 128, :128]
        imag = lines[a * 128 : a * 128 + 128, 128:]
        reals.append(real * cosine - imag * sine)
        imags.append(imag * cosine + real * sine)
    stacked = jnp.concatenate(
        (jnp.concatenate(reals, axis=1), jnp.concatenate(imags, axis=1)), axis=0
    )
    high, low = two_terms(stacked)
    return jnp.dot(
        thrice(table, 1), jnp.concatenate((high, high, low), axis=0), preferred_element_type=f32
    )


def exchange_kernel(scale, call, counts, received, *refs):
    left, right, twiddle, *rest = refs[SOURCES[call] :]
    group, y_at, k2, k, core = place()
    if call < 2:
        source = refs[0] if call else received
        partners = [lambda rows, at=at: source[rows, at] for at in BAND_ROWS]
    else:
        partners = [lambda rows, ref=ref: ref[rows] for ref in refs[:2]]
    if call == 0:
        total, screen = rest
        screen_of(received, refs[0], core, scale, screen)
        held = None
    else:
        screen, held, total = rest
    k2_at = lax.rem(group + 8 - k2 // 2, 8) * 2 + k2 % 2
    core_from = 1 - core if call % 2 else core
    bands = (
        y_band(1 - y_at if call >= 2 else y_at, core_from),
        z_band(y_at, 1 - k if call >= 2 else k, core_from),
    )
    lane = lax.broadcasted_iota(jnp.int32, (1, 16), 1)

    def count_of(kpoint):
        return jnp.sum(jnp.where(lane == kpoint, counts[...].astype(f32), 0.0), axis=1, keepdims=True)

    count = count_of(k2_at)
    kept = [
        jnp.where(count > band.astype(f32), 1.0, 0.0).reshape(1, 1, 1) for band in bands
    ]
    others, chains = [], []
    for half in range(2):
        other = partners[half](slice(0, 32)).astype(f32)
        other_real, other_imag = other[:, :8], other[:, 8:]
        sums, gaps = [[], []], [[], []]
        for a in range(2):
            own = received[:, OWN_ROWS[a]].astype(f32)
            own_real, own_imag = own[:, :8], own[:, 8:]
            density = (
                own_real * other_real + own_imag * other_imag,
                own_imag * other_real - own_real * other_imag,
            )
            for part in range(2):
                low, high = density[part][:16], density[part][16:]
                sums[part].append((low + high).reshape(128, 128))
                gaps[part].append((low - high).reshape(128, 128))
        others.append((half, kept[half]))
        chains += [(0, sums), (1, gaps)]
    cosine, sine = twiddle[0], twiddle[1]
    values = [enter(parts, left[parity]) for parity, parts in chains]
    values = [across(value, right[0], cosine, sine) for value in values]
    values = [
        screened(value, screen[parity], right[1])
        for value, (parity, parts) in zip(values, chains)
    ]
    values = [
        leave(value, left[2 + parity], cosine, sine)
        for value, (parity, parts) in zip(values, chains)
    ]
    backs = [values[2 * half : 2 * half + 2] for half in range(2)]
    for side in range(2):
        rows = slice(side * 16, side * 16 + 16)
        for a in range(2):
            add_real, add_imag = 0.0, 0.0
            if held is not None:
                add_real, add_imag = held[rows, 2 * a], held[rows, 2 * a + 1]
            for (even, odd), (half, factor) in zip(backs, others):
                field = even + odd if side == 0 else even - odd
                other = partners[half](rows).astype(f32) * factor
                b_real, b_imag = other[:, :8], other[:, 8:]
                real = field[:128, a * 128 : a * 128 + 128].reshape(16, 8, 128)
                imag = field[128:, a * 128 : a * 128 + 128].reshape(16, 8, 128)
                add_real += b_real * real - b_imag * imag
                add_imag += b_real * imag + b_imag * real
            total[rows, 2 * a] = add_real
            total[rows, 2 * a + 1] = add_imag


def energy_kernel(counts, received, total, energy):
    group, y_at, k2, k, core = place()
    lane = lax.broadcasted_iota(jnp.int32, (1, 16), 1)
    count = jnp.sum(
        jnp.where(lane == group * 2 + k, counts[...].astype(f32), 0.0), axis=1, keepdims=True
    )
    energy_sum = jnp.zeros((8, 128), f32)
    for a in range(2):
        band = y_at * 4 + core * 2 + a
        occupied = jnp.where(count > band.astype(f32), 1.0, 0.0)
        own = received[:, OWN_ROWS[a]].astype(f32)
        both = own[:, :8] * total[:, 2 * a] + own[:, 8:] * total[:, 2 * a + 1]
        energy_sum += jnp.sum(both, axis=0) * occupied
    energy[...] = jnp.full((8, 128), jnp.sum(energy_sum) * (1.0 / (32.0 * 32768.0)), f32)


def energy_part(counts, received, total):
    vmem = pl.BlockSpec(memory_space=pltpu.VMEM)
    return pl.pallas_call(
        energy_kernel,
        out_shape=jax.ShapeDtypeStruct((8, 128), f32),
        in_specs=[vmem] * 3,
        out_specs=vmem,
        compiler_params=pltpu.CompilerParams(vmem_limit_bytes=4 * MIB),
        name="energy_part",
    )(counts, received, total)


SOURCES = (1, 1, 2, 2)


def exchange(scale, call, counts, received, partners, tables, *carried):
    vmem = pl.BlockSpec(memory_space=pltpu.VMEM)
    operands = (counts, received, *partners, *tables, *carried)
    shapes = [jax.ShapeDtypeStruct((32, 4, 8, 128), f32)]
    if call == 0:
        shapes.append(jax.ShapeDtypeStruct((2, 128, 128), f32))
    return pl.pallas_call(
        functools.partial(exchange_kernel, scale, call),
        out_shape=tuple(shapes),
        in_specs=[vmem] * len(operands),
        out_specs=(vmem,) * len(shapes),
        compiler_params=pltpu.CompilerParams(vmem_limit_bytes=24 * MIB),
        cost_estimate=pl.CostEstimate(
            flops=2 * 12 * 2 * 512 * 256 * 256, bytes_accessed=4 << 20, transcendentals=0
        ),
        name=("exchange_0", "exchange_1", "exchange_2", "exchange_3")[call],
    )(*operands)


def finish_kernel(returned, orbitals, energies, vectors, message):
    fields = []
    for k in range(2):
        for y_at in range(2):
            fields.append(sum(returned[y_at, k2, k] for k2 in range(4)))
    fields = jnp.concatenate(fields, axis=0)
    vectors[...] = fields
    lane = lax.broadcasted_iota(jnp.int32, (8, 128), 1)
    rows = []
    for k in range(2):
        left = jnp.concatenate(
            [orbitals[k * 8 : k * 8 + 8, row] for row in range(16)], axis=1
        ).astype(f32)
        own = fields[k * 16 : k * 16 + 16].reshape(8, 2, 8, 128)
        real = [own[:, 0, row] for row in range(8)]
        imag = [own[:, 1, row] for row in range(8)]
        right = jnp.concatenate(
            (
                jnp.concatenate(real + imag, axis=1),
                jnp.concatenate(imag + [-value for value in real], axis=1),
            ),
            axis=0,
        )
        left = left.astype(bf16)
        product = jnp.zeros((8, 16), f32)
        for _ in range(3):
            term = right.astype(bf16)
            right = right - term.astype(f32)
            product += lax.dot_general(
                left, term, (((1,), (1,)), ((), ())), preferred_element_type=f32
            )
        spread = jnp.concatenate([product * (1.0 / 32768.0)] * 8, axis=1)
        row_at = lax.broadcasted_iota(jnp.int32, (8, 128), 0)
        spread = jnp.where(lane // 16 == row_at, spread, 0.0)
        rows.append(jnp.sum(spread, axis=0, keepdims=True))
    total = energies[:1]
    rows = jnp.concatenate((*rows, total, total), axis=0)
    message[...] = jnp.broadcast_to(rows[None], (32, 4, 128))


def finish(returned, orbitals, energies):
    vmem = pl.BlockSpec(memory_space=pltpu.VMEM)
    return pl.pallas_call(
        finish_kernel,
        out_shape=(
            jax.ShapeDtypeStruct((32, 8, 128), f32),
            jax.ShapeDtypeStruct((32, 4, 128), f32),
        ),
        in_specs=[vmem] * 3,
        out_specs=(vmem, vmem),
        compiler_params=pltpu.CompilerParams(vmem_limit_bytes=8 * MIB),
        name="finish",
    )(returned, orbitals, energies)


def close_kernel(messages, matrix, energy):
    total = jnp.sum(messages[...], axis=0)
    lane = lax.broadcasted_iota(jnp.int32, (32, 128), 1)
    row = lax.broadcasted_iota(jnp.int32, (32, 128), 0)
    spread = jnp.concatenate(
        [jnp.broadcast_to(total[k : k + 1], (16, 128)) for k in range(2)], axis=0
    )
    spread = jnp.where(lane // 8 == row % 8 * 2 + row // 8 % 2, spread, 0.0)
    gather = jnp.where(
        lax.broadcasted_iota(jnp.int32, (128, 128), 0) % 8
        == lax.broadcasted_iota(jnp.int32, (128, 128), 1),
        1.0,
        0.0,
    )
    spread = jnp.dot(spread, gather, precision=highest, preferred_element_type=f32)
    for k in range(2):
        for part in range(2):
            first = k * 16 + part * 8
            matrix[k, part] = spread[first : first + 8, :8]
    energy[...] = total[2:3, :1]


def close(messages):
    vmem = pl.BlockSpec(memory_space=pltpu.VMEM)
    return pl.pallas_call(
        close_kernel,
        out_shape=(jax.ShapeDtypeStruct((2, 2, 8, 8), f32), jax.ShapeDtypeStruct((1, 1), f32)),
        in_specs=[vmem],
        out_specs=(vmem, vmem),
        compiler_params=pltpu.CompilerParams(vmem_limit_bytes=4 * MIB),
        name="close",
    )(messages)


def on_device(orbitals, band_counts, pair_slot, kernel):
    left, right, twiddle = (jnp.asarray(table) for table in constants())
    groups = lax.axis_size("ka")
    scale = -1.0 / (16.0 * 32768.0)

    before = lax.ppermute(orbitals, "ka", [(i, (i + 1) % groups) for i in range(groups)])
    chosen = choose(pair_slot, kernel.reshape(16, 8, 128))
    counts = band_counts.reshape(1, 16)
    orbitals = orbitals.reshape(16, 16, 128)
    packed = pack(orbitals, before.reshape(16, 16, 128), chosen)
    received = lax.all_to_all(packed, "ga", 0, 0, tiled=True)

    def shown(value, bit):
        return lax.ppermute(value, "ga", [(i, i ^ bit) for i in range(32)])

    tables = (left, right, twiddle)
    next_core = shown(received[:, :40], 1)
    next_y, next_z = shown(received[:, BAND_ROWS[0]], 16), shown(received[:, BAND_ROWS[1]], 2)
    total, screen = exchange(scale, 0, counts, received, (next_core,), tables)
    (total,) = exchange(scale, 1, counts, received, (next_core,), tables, screen, total)
    next_y, next_z, total = lax.optimization_barrier((next_y, next_z, total))
    far = (shown(next_y, 1), shown(next_z, 1))
    (total,) = exchange(scale, 2, counts, received, (next_y, next_z), tables, screen, total)
    (total,) = exchange(scale, 3, counts, received, far, tables, screen, total)

    returned = lax.all_to_all(total, "ga", 0, 0, tiled=True)
    energy = energy_part(counts, received, total)
    shown_energy = lambda value, bit: lax.ppermute(value, "ka", [(i, i ^ bit) for i in range(groups)])
    near = [shown_energy(energy, bit) for bit in (1, 2, 3)]
    energy = (energy + near[0]) + (near[1] + near[2])
    energy = energy + shown_energy(energy, 4)
    vectors, message = finish(returned.reshape(2, 4, 2, 8, 8, 128), orbitals, energy)
    matrix, energy = close(lax.all_to_all(message, "ga", 0, 0, tiled=True))
    return (vectors.reshape(2, 8, 2, 1, 1024), matrix, energy[0, 0])


def solution(mesh):
    in_specs = (P("ka", None, None, "ga", None), P(), P(), P(None, None, "ga"))
    out_specs = (P("ka", None, None, "ga", None), P("ka", None, None, None), P())
    return jax.shard_map(
        on_device, mesh=mesh, in_specs=in_specs, out_specs=out_specs, check_vma=False
    )
```

```python
import functools

import numpy as np
import jax
import jax.numpy as jnp
from jax import lax
from jax.experimental import pallas as pl
from jax.experimental.pallas import tpu as pltpu
from jax.sharding import PartitionSpec as P

highest = lax.Precision.HIGHEST
f32 = jnp.float32
bf16 = jnp.bfloat16


def embed(matrix):
    return np.block([[matrix.real, -matrix.imag], [matrix.imag, matrix.real]])


def split(matrix):
    high = matrix.astype(np.float32).astype(bf16)
    low = (matrix - high.astype(np.float64)).astype(np.float32).astype(bf16)
    return high, low


def constants():
    rows = np.arange(128)
    x_at, yh_at = rows // 8, rows % 8
    jj_at, glo_at, gxh_at = rows // 64, rows // 8 % 8, rows % 8
    forward, inverse = [], []
    for parity in range(2):
        gx_at = 4 * gxh_at + 2 * jj_at + parity
        phase = gx_at[:, None] * x_at[None, :] / 32.0 + glo_at[:, None] * yh_at[None, :] / 8.0
        real = embed(np.exp(-2j * np.pi * phase))
        for held, matrix in ((forward, real), (inverse, real.T)):
            high, low = split(matrix)
            held.append(np.concatenate((high, low), axis=1))
    lanes = np.arange(128)
    first, last = lanes // 32, lanes % 32
    phase = first[:, None] * first[None, :] / 4.0 + last[:, None] * last[None, :] / 32.0
    real = embed(np.exp(-2j * np.pi * phase)).T
    right = []
    for matrix in (real, real.T):
        high, low = split(matrix)
        right.append(np.concatenate((high, low), axis=0))
    turn = 2.0 * np.pi * (glo_at[:, None] * first[None, :]) / 32.0
    twiddle = np.stack((np.cos(turn), np.sin(turn))).astype(np.float32)
    return np.stack(forward + inverse), np.stack(right), twiddle


def two_terms(value):
    high = value.astype(bf16)
    low = (value - high.astype(f32)).astype(bf16)
    return high, low


MIB = 1 << 20


def place():
    member = lax.axis_index("ga")
    return lax.axis_index("ka"), member // 16, member // 4 % 4, member // 2 % 2, member % 2


def y_band(y_at, core):
    return 4 * y_at + core


def z_band(y_at, k, core):
    return 2 + 4 * ((y_at + k) % 2) + core


def choose_kernel(pair_slot, kernel, chosen):
    group = lax.axis_index("ka")
    partner_group = lax.rem(group + 7, 8)
    for k2 in range(4):
        second = (group if k2 < 2 else partner_group) * 2 + k2 % 2
        for k in range(2):
            block = kernel[pair_slot[group * 2 + k, second]]
            high, low = two_terms(block)
            for core in range(2):
                rows = slice(core * 4, core * 4 + 4)
                chosen[k2 * 2 + k, core] = jnp.concatenate((high[rows], low[rows]), axis=0)


def choose(pair_slot, kernel):
    vmem = pl.BlockSpec(memory_space=pltpu.VMEM)
    return pl.pallas_call(
        choose_kernel,
        out_shape=jax.ShapeDtypeStruct((8, 2, 8, 128), bf16),
        in_specs=[pl.BlockSpec(memory_space=pltpu.SMEM), vmem],
        out_specs=vmem,
        compiler_params=pltpu.CompilerParams(vmem_limit_bytes=4 * MIB),
        name="choose",
    )(pair_slot, kernel)


KERNEL_ROWS = slice(0, 8)
BAND_ROWS = (slice(8, 24), slice(24, 40))
OWN_ROWS = (slice(40, 56), slice(56, 72))


def pack_kernel(orbitals, before, chosen, packed):
    for k2 in range(4):
        source = orbitals if k2 < 2 else before
        for k in range(2):
            for quarter in range(4):
                y_at, core = quarter // 2, quarter % 2
                to = y_at * 16 + k2 * 4 + k * 2 + core
                packed[to, KERNEL_ROWS] = chosen[k2 * 2 + k, core]
                packed[to, BAND_ROWS[0]] = source[k2 % 2 * 8 + y_band(y_at, core)]
                packed[to, BAND_ROWS[1]] = source[k2 % 2 * 8 + z_band(y_at, k, core)]
                for j in range(2):
                    packed[to, OWN_ROWS[j]] = orbitals[k * 8 + quarter * 2 + j]


def pack(orbitals, before, chosen):
    vmem = pl.BlockSpec(memory_space=pltpu.VMEM)
    return pl.pallas_call(
        pack_kernel,
        out_shape=jax.ShapeDtypeStruct((32, 72, 128), bf16),
        in_specs=[vmem, vmem, vmem],
        out_specs=vmem,
        compiler_params=pltpu.CompilerParams(vmem_limit_bytes=4 * MIB),
        name="pack",
    )(orbitals, before, chosen)


def screen_of(received, other, core, scale, screen):
    halves = []
    for half in (received, other):
        half = half[:, KERNEL_ROWS].astype(f32)
        halves.append(((half + pltpu.roll(half, 4, 1)) * scale).reshape(256, 128))
    row = lax.broadcasted_iota(jnp.int32, (256, 128), 0) % 8
    raw = jnp.where(row // 4 == core, halves[0], halves[1]).reshape(4, 64, 128)
    lane_group = lax.broadcasted_iota(jnp.int32, (64, 128), 1) // 32
    for j in range(4):
        placed = jnp.zeros((64, 128), f32)
        for i in range(4):
            shift = (i - j) % 4 * 32
            moved = pltpu.roll(raw[i], shift, 1) if shift else raw[i]
            placed = jnp.where(lane_group == i, moved, placed)
        screen[j % 2, (j // 2) * 64 : (j // 2) * 64 + 64] = placed


def thrice(table, axis):
    size = table.shape[axis] // 2
    return jnp.concatenate((table, lax.slice_in_dim(table, 0, size, axis=axis)), axis=axis)


def enter(parts, table):
    stacked = jnp.concatenate([jnp.concatenate(parts[part], axis=1) for part in range(2)], axis=0)
    high, low = two_terms(stacked)
    return jnp.dot(
        thrice(table, 1), jnp.concatenate((high, high, low), axis=0), preferred_element_type=f32
    )


def across(turned, table, cosine, sine):
    lines = []
    for a in range(2):
        real = turned[:128, a * 128 : a * 128 + 128]
        imag = turned[128:, a * 128 : a * 128 + 128]
        lines.append(
            jnp.concatenate((real * cosine + imag * sine, imag * cosine - real * sine), axis=1)
        )
    high, low = two_terms(jnp.concatenate(lines, axis=0))
    return jnp.dot(
        jnp.concatenate((high, high, low), axis=1), thrice(table, 0), preferred_element_type=f32
    )


def screened(spectra, factor, table):
    factor = jnp.concatenate((factor, factor), axis=1)
    factor = jnp.concatenate((factor, factor), axis=0)
    high, low = two_terms(spectra * factor)
    return jnp.dot(
        jnp.concatenate((high, high, low), axis=1), thrice(table, 0), preferred_element_type=f32
    )


def leave(lines, table, cosine, sine):
    reals, imags = [], []
    for a in range(2):
        real = lines[a * 128 : a * 128 + 128, :128]
        imag = lines[a * 128 : a * 128 + 128, 128:]
        reals.append(real * cosine - imag * sine)
        imags.append(imag * cosine + real * sine)
    stacked = jnp.concatenate(
        (jnp.concatenate(reals, axis=1), jnp.concatenate(imags, axis=1)), axis=0
    )
    high, low = two_terms(stacked)
    return jnp.dot(
        thrice(table, 1), jnp.concatenate((high, high, low), axis=0), preferred_element_type=f32
    )


LEVELS = 10
BASE = 2 * LEVELS + 1


def remainder(value):
    high = value.astype(bf16)
    wide = high.astype(f32)
    share = (value - wide) / jnp.where(wide == 0.0, 1.0, wide)
    return high, jnp.floor(share * (256.0 * LEVELS) + 0.5)


def coded(real, imag):
    real, first = remainder(real)
    imag, second = remainder(imag)
    return jnp.concatenate((real, imag), axis=1), first * BASE + second


def decoded(high, code):
    first = jnp.floor(code * (1.0 / BASE) + 0.5)
    second = code - first * BASE
    step = 1.0 / (256.0 * LEVELS)
    return high[..., :8, :] * (1.0 + first * step), high[..., 8:, :] * (1.0 + second * step)


def exchange_kernel(scale, call, counts, received, *refs):
    left, right, twiddle, *rest = refs[SOURCES[call] :]
    group, y_at, k2, k, core = place()
    if call < 2:
        source = refs[0] if call else received
        partners = [lambda rows, at=at: source[rows, at] for at in BAND_ROWS]
    else:
        partners = [lambda rows, ref=ref: ref[rows] for ref in refs[:2]]
    if call == 0:
        total, screen = rest
        screen_of(received, refs[0], core, scale, screen)
        held = None
    else:
        screen, held, total = rest[:3]
        if call == 3:
            leaving, energy, total = rest[2:]
    k2_at = lax.rem(group + 8 - k2 // 2, 8) * 2 + k2 % 2
    core_from = 1 - core if call % 2 else core
    bands = (
        y_band(1 - y_at if call >= 2 else y_at, core_from),
        z_band(y_at, 1 - k if call >= 2 else k, core_from),
    )
    lane = lax.broadcasted_iota(jnp.int32, (1, 16), 1)

    def count_of(kpoint):
        return jnp.sum(jnp.where(lane == kpoint, counts[...].astype(f32), 0.0), axis=1, keepdims=True)

    count = count_of(k2_at)
    kept = [
        jnp.where(count > band.astype(f32), 1.0, 0.0).reshape(1, 1, 1) for band in bands
    ]
    others, chains = [], []
    for half in range(2):
        other = partners[half](slice(0, 32)).astype(f32)
        other_real, other_imag = other[:, :8], other[:, 8:]
        sums, gaps = [[], []], [[], []]
        for a in range(2):
            own = received[:, OWN_ROWS[a]].astype(f32)
            own_real, own_imag = own[:, :8], own[:, 8:]
            density = (
                own_real * other_real + own_imag * other_imag,
                own_imag * other_real - own_real * other_imag,
            )
            for part in range(2):
                low, high = density[part][:16], density[part][16:]
                sums[part].append((low + high).reshape(128, 128))
                gaps[part].append((low - high).reshape(128, 128))
        others.append((half, kept[half]))
        chains += [(0, sums), (1, gaps)]
    cosine, sine = twiddle[0], twiddle[1]
    values = [enter(parts, left[parity]) for parity, parts in chains]
    values = [across(value, right[0], cosine, sine) for value in values]
    values = [
        screened(value, screen[parity], right[1])
        for value, (parity, parts) in zip(values, chains)
    ]
    values = [
        leave(value, left[2 + parity], cosine, sine)
        for value, (parity, parts) in zip(values, chains)
    ]
    backs = [values[2 * half : 2 * half + 2] for half in range(2)]
    for side in range(2):
        rows = slice(side * 16, side * 16 + 16)
        codes = []
        for a in range(2):
            add_real, add_imag = 0.0, 0.0
            if held is not None:
                add_real, add_imag = held[rows, 2 * a], held[rows, 2 * a + 1]
            for (even, odd), (half, factor) in zip(backs, others):
                field = even + odd if side == 0 else even - odd
                other = partners[half](rows).astype(f32) * factor
                b_real, b_imag = other[:, :8], other[:, 8:]
                real = field[:128, a * 128 : a * 128 + 128].reshape(16, 8, 128)
                imag = field[128:, a * 128 : a * 128 + 128].reshape(16, 8, 128)
                add_real += b_real * real - b_imag * imag
                add_imag += b_real * imag + b_imag * real
            total[rows, 2 * a] = add_real
            total[rows, 2 * a + 1] = add_imag
            if call == 3:
                leaving[rows, 16 * a : 16 * a + 16], code = coded(add_real, add_imag)
                codes.append(code)
        if call == 3:
            leaving[rows, 32:48] = jnp.concatenate(codes, axis=1).astype(bf16)

    if call == 3:
        count = count_of(group * 2 + k)
        energy_sum = jnp.zeros((8, 128), f32)
        for a in range(2):
            occupied = jnp.where(count > (y_at * 4 + core * 2 + a).astype(f32), 1.0, 0.0)
            own = received[:, OWN_ROWS[a]].astype(f32)
            both = own[:, :8] * total[:, 2 * a] + own[:, 8:] * total[:, 2 * a + 1]
            energy_sum += jnp.sum(both, axis=0) * occupied
        energy[...] = jnp.full((8, 128), jnp.sum(energy_sum) * (1.0 / (32.0 * 32768.0)), f32)


SOURCES = (1, 1, 2, 2)


def exchange(scale, call, counts, received, partners, tables, *carried):
    vmem = pl.BlockSpec(memory_space=pltpu.VMEM)
    operands = (counts, received, *partners, *tables, *carried)
    shapes, scratch = [jax.ShapeDtypeStruct((32, 4, 8, 128), f32)], []
    if call == 3:
        shapes = [jax.ShapeDtypeStruct((32, 48, 128), bf16), jax.ShapeDtypeStruct((8, 128), f32)]
        scratch = [pltpu.VMEM((32, 4, 8, 128), f32)]
    if call == 0:
        shapes.append(jax.ShapeDtypeStruct((2, 128, 128), f32))
    return pl.pallas_call(
        functools.partial(exchange_kernel, scale, call),
        out_shape=tuple(shapes),
        in_specs=[vmem] * len(operands),
        out_specs=(vmem,) * len(shapes),
        scratch_shapes=scratch,
        compiler_params=pltpu.CompilerParams(vmem_limit_bytes=24 * MIB),
        cost_estimate=pl.CostEstimate(
            flops=2 * 12 * 2 * 512 * 256 * 256, bytes_accessed=4 << 20, transcendentals=0
        ),
        name=("exchange_0", "exchange_1", "exchange_2", "exchange_3")[call],
    )(*operands)


def finish_kernel(returned, orbitals, energies, vectors, message):
    fields = []
    for k in range(2):
        for y_at in range(2):
            for core in range(2):
                sums = [0.0] * 4
                for k2 in range(4):
                    block = returned[y_at, k2, k, core].astype(f32)
                    for a in range(2):
                        parts = decoded(
                            block[16 * a : 16 * a + 16], block[32 + 8 * a : 40 + 8 * a]
                        )
                        for part in range(2):
                            sums[2 * a + part] += parts[part]
                fields += [value.reshape(1, 8, 128) for value in sums]
    fields = jnp.concatenate(fields, axis=0)
    vectors[...] = fields
    lane = lax.broadcasted_iota(jnp.int32, (8, 128), 1)
    rows = []
    for k in range(2):
        left = jnp.concatenate(
            [orbitals[k * 8 : k * 8 + 8, row] for row in range(16)], axis=1
        ).astype(f32)
        own = fields[k * 16 : k * 16 + 16].reshape(8, 2, 8, 128)
        real = [own[:, 0, row] for row in range(8)]
        imag = [own[:, 1, row] for row in range(8)]
        right = jnp.concatenate(
            (
                jnp.concatenate(real + imag, axis=1),
                jnp.concatenate(imag + [-value for value in real], axis=1),
            ),
            axis=0,
        )
        left = left.astype(bf16)
        product = jnp.zeros((8, 16), f32)
        for _ in range(3):
            term = right.astype(bf16)
            right = right - term.astype(f32)
            product += lax.dot_general(
                left, term, (((1,), (1,)), ((), ())), preferred_element_type=f32
            )
        spread = jnp.concatenate([product * (1.0 / 32768.0)] * 8, axis=1)
        row_at = lax.broadcasted_iota(jnp.int32, (8, 128), 0)
        spread = jnp.where(lane // 16 == row_at, spread, 0.0)
        rows.append(jnp.sum(spread, axis=0, keepdims=True))
    total = energies[:1]
    rows = jnp.concatenate((*rows, total, total), axis=0)
    message[...] = jnp.broadcast_to(rows[None], (32, 4, 128))


def finish(returned, orbitals, energies):
    vmem = pl.BlockSpec(memory_space=pltpu.VMEM)
    return pl.pallas_call(
        finish_kernel,
        out_shape=(
            jax.ShapeDtypeStruct((32, 8, 128), f32),
            jax.ShapeDtypeStruct((32, 4, 128), f32),
        ),
        in_specs=[vmem] * 3,
        out_specs=(vmem, vmem),
        compiler_params=pltpu.CompilerParams(vmem_limit_bytes=8 * MIB),
        name="finish",
    )(returned, orbitals, energies)


def close_kernel(messages, matrix, energy):
    total = jnp.sum(messages[...], axis=0)
    lane = lax.broadcasted_iota(jnp.int32, (32, 128), 1)
    row = lax.broadcasted_iota(jnp.int32, (32, 128), 0)
    spread = jnp.concatenate(
        [jnp.broadcast_to(total[k : k + 1], (16, 128)) for k in range(2)], axis=0
    )
    spread = jnp.where(lane // 8 == row % 8 * 2 + row // 8 % 2, spread, 0.0)
    gather = jnp.where(
        lax.broadcasted_iota(jnp.int32, (128, 128), 0) % 8
        == lax.broadcasted_iota(jnp.int32, (128, 128), 1),
        1.0,
        0.0,
    )
    spread = jnp.dot(spread, gather, precision=highest, preferred_element_type=f32)
    for k in range(2):
        for part in range(2):
            first = k * 16 + part * 8
            matrix[k, part] = spread[first : first + 8, :8]
    energy[...] = total[2:3, :1]


def close(messages):
    vmem = pl.BlockSpec(memory_space=pltpu.VMEM)
    return pl.pallas_call(
        close_kernel,
        out_shape=(jax.ShapeDtypeStruct((2, 2, 8, 8), f32), jax.ShapeDtypeStruct((1, 1), f32)),
        in_specs=[vmem],
        out_specs=(vmem, vmem),
        compiler_params=pltpu.CompilerParams(vmem_limit_bytes=4 * MIB),
        name="close",
    )(messages)


def on_device(orbitals, band_counts, pair_slot, kernel):
    left, right, twiddle = (jnp.asarray(table) for table in constants())
    groups = lax.axis_size("ka")
    scale = -1.0 / (16.0 * 32768.0)

    before = lax.ppermute(orbitals, "ka", [(i, (i + 1) % groups) for i in range(groups)])
    chosen = choose(pair_slot, kernel.reshape(16, 8, 128))
    counts = band_counts.reshape(1, 16)
    orbitals = orbitals.reshape(16, 16, 128)
    packed = pack(orbitals, before.reshape(16, 16, 128), chosen)
    received = lax.all_to_all(packed, "ga", 0, 0, tiled=True)

    def shown(value, bit):
        return lax.ppermute(value, "ga", [(i, i ^ bit) for i in range(32)])

    tables = (left, right, twiddle)
    next_core = shown(received[:, :40], 1)
    next_y, next_z = shown(received[:, BAND_ROWS[0]], 16), shown(received[:, BAND_ROWS[1]], 2)
    total, screen = exchange(scale, 0, counts, received, (next_core,), tables)
    (total,) = exchange(scale, 1, counts, received, (next_core,), tables, screen, total)
    next_y, next_z, total = lax.optimization_barrier((next_y, next_z, total))
    far = (shown(next_y, 1), shown(next_z, 1))
    (total,) = exchange(scale, 2, counts, received, (next_y, next_z), tables, screen, total)
    leaving, energy = exchange(scale, 3, counts, received, far, tables, screen, total)

    returned = lax.all_to_all(leaving, "ga", 0, 0, tiled=True)
    shown_energy = lambda value, bit: lax.ppermute(value, "ka", [(i, i ^ bit) for i in range(groups)])
    near = [shown_energy(energy, bit) for bit in (1, 2, 3)]
    energy = (energy + near[0]) + (near[1] + near[2])
    energy = energy + shown_energy(energy, 4)
    vectors, message = finish(returned.reshape(2, 4, 2, 2, 48, 128), orbitals, energy)
    matrix, energy = close(lax.all_to_all(message, "ga", 0, 0, tiled=True))
    return (vectors.reshape(2, 8, 2, 1, 1024), matrix, energy[0, 0])


def solution(mesh):
    in_specs = (P("ka", None, None, "ga", None), P(), P(), P(None, None, "ga"))
    out_specs = (P("ka", None, None, "ga", None), P("ka", None, None, None), P())
    return jax.shard_map(
        on_device, mesh=mesh, in_specs=in_specs, out_specs=out_specs, check_vma=False
    )
```

```python
import functools

import numpy as np
import jax
import jax.numpy as jnp
from jax import lax
from jax.experimental import pallas as pl
from jax.experimental.pallas import tpu as pltpu
from jax.sharding import PartitionSpec as P


highest = lax.Precision.HIGHEST
f32 = jnp.float32
bf16 = jnp.bfloat16


def embed(matrix):
    return np.block([[matrix.real, -matrix.imag], [matrix.imag, matrix.real]])


def split(matrix):
    high = matrix.astype(np.float32).astype(bf16)
    low = (matrix - high.astype(np.float64)).astype(np.float32).astype(bf16)
    return high, low


def constants():
    rows = np.arange(128)
    x_at, yh_at = rows // 8, rows % 8
    jj_at, glo_at, gxh_at = rows // 64, rows // 8 % 8, rows % 8
    forward, inverse = [], []
    for parity in range(2):
        gx_at = 4 * gxh_at + 2 * jj_at + parity
        phase = gx_at[:, None] * x_at[None, :] / 32.0 + glo_at[:, None] * yh_at[None, :] / 8.0
        real = embed(np.exp(-2j * np.pi * phase))
        for held, matrix in ((forward, real), (inverse, real.T)):
            high, low = split(matrix)
            held.append(np.concatenate((high, low), axis=1))
    lanes = np.arange(128)
    first, last = lanes // 32, lanes % 32
    phase = first[:, None] * first[None, :] / 4.0 + last[:, None] * last[None, :] / 32.0
    real = embed(np.exp(-2j * np.pi * phase)).T
    right = []
    for matrix in (real, real.T):
        high, low = split(matrix)
        right.append(np.concatenate((high, low), axis=0))
    turn = 2.0 * np.pi * (glo_at[:, None] * first[None, :]) / 32.0
    twiddle = np.stack((np.cos(turn), np.sin(turn))).astype(np.float32)
    return np.stack(forward + inverse), np.stack(right), twiddle


def two_terms(value):
    high = value.astype(bf16)
    low = (value - high.astype(f32)).astype(bf16)
    return high, low


MIB = 1 << 20


def place():
    member = lax.axis_index("ga")
    return lax.axis_index("ka"), member // 16, member // 4 % 4, member // 2 % 2, member % 2


def y_band(y_at, core):
    return 4 * y_at + core


def z_band(y_at, k, core):
    return 2 + 4 * ((y_at + k) % 2) + core


def choose_kernel(pair_slot, kernel, chosen):
    group = lax.axis_index("ka")
    partner_group = lax.rem(group + 7, 8)
    for k2 in range(4):
        second = (group if k2 < 2 else partner_group) * 2 + k2 % 2
        for k in range(2):
            block = kernel[pair_slot[group * 2 + k, second]]
            high, low = two_terms(block)
            for core in range(2):
                rows = slice(core * 4, core * 4 + 4)
                chosen[k2 * 2 + k, core] = jnp.concatenate((high[rows], low[rows]), axis=0)


def choose(pair_slot, kernel):
    vmem = pl.BlockSpec(memory_space=pltpu.VMEM)
    return pl.pallas_call(
        choose_kernel,
        out_shape=jax.ShapeDtypeStruct((8, 2, 8, 128), bf16),
        in_specs=[pl.BlockSpec(memory_space=pltpu.SMEM), vmem],
        out_specs=vmem,
        compiler_params=pltpu.CompilerParams(vmem_limit_bytes=4 * MIB),
        name="choose",
    )(pair_slot, kernel)


KERNEL_ROWS = slice(0, 8)
BAND_ROWS = (slice(8, 24), slice(24, 40))
OWN_ROWS = (slice(40, 56), slice(56, 72))


def pack_kernel(orbitals, before, chosen, packed):
    for k2 in range(4):
        source = orbitals if k2 < 2 else before
        for k in range(2):
            for quarter in range(4):
                y_at, core = quarter // 2, quarter % 2
                to = y_at * 16 + k2 * 4 + k * 2 + core
                packed[to, KERNEL_ROWS] = chosen[k2 * 2 + k, core]
                packed[to, BAND_ROWS[0]] = source[k2 % 2 * 8 + y_band(y_at, core)]
                packed[to, BAND_ROWS[1]] = source[k2 % 2 * 8 + z_band(y_at, k, core)]
                for j in range(2):
                    packed[to, OWN_ROWS[j]] = orbitals[k * 8 + quarter * 2 + j]


def pack(orbitals, before, chosen):
    vmem = pl.BlockSpec(memory_space=pltpu.VMEM)
    return pl.pallas_call(
        pack_kernel,
        out_shape=jax.ShapeDtypeStruct((32, 72, 128), bf16),
        in_specs=[vmem, vmem, vmem],
        out_specs=vmem,
        compiler_params=pltpu.CompilerParams(vmem_limit_bytes=4 * MIB),
        name="pack",
    )(orbitals, before, chosen)


def screen_of(received, other, core, scale, screen):
    halves = []
    for half in (received, other):
        half = half[:, KERNEL_ROWS].astype(f32)
        halves.append(((half + pltpu.roll(half, 4, 1)) * scale).reshape(256, 128))
    row = lax.broadcasted_iota(jnp.int32, (256, 128), 0) % 8
    raw = jnp.where(row // 4 == core, halves[0], halves[1]).reshape(4, 64, 128)
    lane_group = lax.broadcasted_iota(jnp.int32, (64, 128), 1) // 32
    for j in range(4):
        placed = jnp.zeros((64, 128), f32)
        for i in range(4):
            shift = (i - j) % 4 * 32
            moved = pltpu.roll(raw[i], shift, 1) if shift else raw[i]
            placed = jnp.where(lane_group == i, moved, placed)
        screen[j % 2, (j // 2) * 64 : (j // 2) * 64 + 64] = placed


def thrice(table, axis):
    size = table.shape[axis] // 2
    return jnp.concatenate((table, lax.slice_in_dim(table, 0, size, axis=axis)), axis=axis)


def enter(parts, table):
    stacked = jnp.concatenate([jnp.concatenate(parts[part], axis=1) for part in range(2)], axis=0)
    high, low = two_terms(stacked)
    return jnp.dot(
        thrice(table, 1), jnp.concatenate((high, high, low), axis=0), preferred_element_type=f32
    )


def across(turned, table, cosine, sine):
    lines = []
    for a in range(2):
        real = turned[:128, a * 128 : a * 128 + 128]
        imag = turned[128:, a * 128 : a * 128 + 128]
        lines.append(
            jnp.concatenate((real * cosine + imag * sine, imag * cosine - real * sine), axis=1)
        )
    high, low = two_terms(jnp.concatenate(lines, axis=0))
    return jnp.dot(
        jnp.concatenate((high, high, low), axis=1), thrice(table, 0), preferred_element_type=f32
    )


def screened(spectra, factor, table):
    factor = jnp.concatenate((factor, factor), axis=1)
    factor = jnp.concatenate((factor, factor), axis=0)
    high, low = two_terms(spectra * factor)
    return jnp.dot(
        jnp.concatenate((high, high, low), axis=1), thrice(table, 0), preferred_element_type=f32
    )


def leave(lines, table, cosine, sine):
    reals, imags = [], []
    for a in range(2):
        real = lines[a * 128 : a * 128 + 128, :128]
        imag = lines[a * 128 : a * 128 + 128, 128:]
        reals.append(real * cosine - imag * sine)
        imags.append(imag * cosine + real * sine)
    stacked = jnp.concatenate(
        (jnp.concatenate(reals, axis=1), jnp.concatenate(imags, axis=1)), axis=0
    )
    high, low = two_terms(stacked)
    return jnp.dot(
        thrice(table, 1), jnp.concatenate((high, high, low), axis=0), preferred_element_type=f32
    )


LEVELS = 10
BASE = 2 * LEVELS + 1


def remainder(value):
    high = value.astype(bf16)
    wide = high.astype(f32)
    share = (value - wide) / jnp.where(wide == 0.0, 1.0, wide)
    return high, jnp.floor(share * (256.0 * LEVELS) + 0.5)


def coded(real, imag):
    real, first = remainder(real)
    imag, second = remainder(imag)
    return jnp.concatenate((real, imag), axis=1), first * BASE + second


def decoded(high, code):
    first = jnp.floor(code * (1.0 / BASE) + 0.5)
    second = code - first * BASE
    step = 1.0 / (256.0 * LEVELS)
    return high[..., :8, :] * (1.0 + first * step), high[..., 8:, :] * (1.0 + second * step)


def exchange_kernel(scale, call, counts, received, *refs):
    left, right, twiddle, *rest = refs[SOURCES[call] :]
    group, y_at, k2, k, core = place()
    if call < 2:
        source = refs[0] if call else received
        partners = [lambda rows, at=at: source[rows, at] for at in BAND_ROWS]
    else:
        partners = [lambda rows, ref=ref: ref[rows] for ref in refs[:2]]
    if call == 0:
        total, screen = rest
        screen_of(received, refs[0], core, scale, screen)
        held = None
    else:
        screen, held, total = rest[:3]
        if call == 3:
            leaving, energy, total = rest[2:]
    k2_at = lax.rem(group + 8 - k2 // 2, 8) * 2 + k2 % 2
    core_from = 1 - core if call % 2 else core
    bands = (
        y_band(1 - y_at if call >= 2 else y_at, core_from),
        z_band(y_at, 1 - k if call >= 2 else k, core_from),
    )
    lane = lax.broadcasted_iota(jnp.int32, (1, 16), 1)

    def count_of(kpoint):
        return jnp.sum(jnp.where(lane == kpoint, counts[...].astype(f32), 0.0), axis=1, keepdims=True)

    count = count_of(k2_at)
    kept = [
        jnp.where(count > band.astype(f32), 1.0, 0.0).reshape(1, 1, 1) for band in bands
    ]
    others, chains = [], []
    for half in range(2):
        other = partners[half](slice(0, 32)).astype(f32)
        other_real, other_imag = other[:, :8], other[:, 8:]
        sums, gaps = [[], []], [[], []]
        for a in range(2):
            own = received[:, OWN_ROWS[a]].astype(f32)
            own_real, own_imag = own[:, :8], own[:, 8:]
            density = (
                own_real * other_real + own_imag * other_imag,
                own_imag * other_real - own_real * other_imag,
            )
            for part in range(2):
                low, high = density[part][:16], density[part][16:]
                sums[part].append((low + high).reshape(128, 128))
                gaps[part].append((low - high).reshape(128, 128))
        others.append((half, kept[half]))
        chains += [(0, sums), (1, gaps)]
    cosine, sine = twiddle[0], twiddle[1]
    values = [enter(parts, left[parity]) for parity, parts in chains]
    values = [across(value, right[0], cosine, sine) for value in values]
    values = [
        screened(value, screen[parity], right[1])
        for value, (parity, parts) in zip(values, chains)
    ]
    values = [
        leave(value, left[2 + parity], cosine, sine)
        for value, (parity, parts) in zip(values, chains)
    ]
    backs = [values[2 * half : 2 * half + 2] for half in range(2)]
    for side in range(2):
        rows = slice(side * 16, side * 16 + 16)
        codes = []
        for a in range(2):
            add_real, add_imag = 0.0, 0.0
            if held is not None:
                add_real, add_imag = held[rows, 2 * a], held[rows, 2 * a + 1]
            for (even, odd), (half, factor) in zip(backs, others):
                field = even + odd if side == 0 else even - odd
                other = partners[half](rows).astype(f32) * factor
                b_real, b_imag = other[:, :8], other[:, 8:]
                real = field[:128, a * 128 : a * 128 + 128].reshape(16, 8, 128)
                imag = field[128:, a * 128 : a * 128 + 128].reshape(16, 8, 128)
                add_real += b_real * real - b_imag * imag
                add_imag += b_real * imag + b_imag * real
            total[rows, 2 * a] = add_real
            total[rows, 2 * a + 1] = add_imag
            if call == 3:
                leaving[rows, 16 * a : 16 * a + 16], code = coded(add_real, add_imag)
                codes.append(code)
        if call == 3:
            leaving[rows, 32:48] = jnp.concatenate(codes, axis=1).astype(bf16)

    if call == 3:
        count = count_of(group * 2 + k)
        energy_sum = jnp.zeros((8, 128), f32)
        for a in range(2):
            occupied = jnp.where(count > (y_at * 4 + core * 2 + a).astype(f32), 1.0, 0.0)
            own = received[:, OWN_ROWS[a]].astype(f32)
            both = own[:, :8] * total[:, 2 * a] + own[:, 8:] * total[:, 2 * a + 1]
            energy_sum += jnp.sum(both, axis=0) * occupied
        energy[...] = jnp.full((8, 128), jnp.sum(energy_sum) * (1.0 / (32.0 * 32768.0)), f32)


SOURCES = (1, 1, 2, 2)


def exchange(scale, call, counts, received, partners, tables, *carried):
    vmem = pl.BlockSpec(memory_space=pltpu.VMEM)
    operands = (counts, received, *partners, *tables, *carried)
    shapes, scratch = [jax.ShapeDtypeStruct((32, 4, 8, 128), f32)], []
    if call == 3:
        shapes = [jax.ShapeDtypeStruct((32, 48, 128), bf16), jax.ShapeDtypeStruct((8, 128), f32)]
        scratch = [pltpu.VMEM((32, 4, 8, 128), f32)]
    if call == 0:
        shapes.append(jax.ShapeDtypeStruct((2, 128, 128), f32))
    return pl.pallas_call(
        functools.partial(exchange_kernel, scale, call),
        out_shape=tuple(shapes),
        in_specs=[vmem] * len(operands),
        out_specs=(vmem,) * len(shapes),
        scratch_shapes=scratch,
        compiler_params=pltpu.CompilerParams(vmem_limit_bytes=24 * MIB),
        cost_estimate=pl.CostEstimate(
            flops=2 * 12 * 2 * 512 * 256 * 256, bytes_accessed=4 << 20, transcendentals=0
        ),
    )(*operands)


def finish_kernel(returned, orbitals, energies, vectors, message):
    fields = []
    for k in range(2):
        for y_at in range(2):
            for core in range(2):
                sums = [0.0] * 4
                for k2 in range(4):
                    block = returned[y_at, k2, k, core].astype(f32)
                    for a in range(2):
                        parts = decoded(
                            block[16 * a : 16 * a + 16], block[32 + 8 * a : 40 + 8 * a]
                        )
                        for part in range(2):
                            sums[2 * a + part] += parts[part]
                fields += [value.reshape(1, 8, 128) for value in sums]
    fields = jnp.concatenate(fields, axis=0)
    vectors[...] = fields
    lane = lax.broadcasted_iota(jnp.int32, (8, 128), 1)
    rows = []
    for k in range(2):
        left = jnp.concatenate(
            [orbitals[k * 8 : k * 8 + 8, row] for row in range(16)], axis=1
        ).astype(f32)
        own = fields[k * 16 : k * 16 + 16].reshape(8, 2, 8, 128)
        real = [own[:, 0, row] for row in range(8)]
        imag = [own[:, 1, row] for row in range(8)]
        right = jnp.concatenate(
            (
                jnp.concatenate(real + imag, axis=1),
                jnp.concatenate(imag + [-value for value in real], axis=1),
            ),
            axis=0,
        )
        left = left.astype(bf16)
        product = jnp.zeros((8, 16), f32)
        for _ in range(3):
            term = right.astype(bf16)
            right = right - term.astype(f32)
            product += lax.dot_general(
                left, term, (((1,), (1,)), ((), ())), preferred_element_type=f32
            )
        spread = jnp.concatenate([product * (1.0 / 32768.0)] * 8, axis=1)
        row_at = lax.broadcasted_iota(jnp.int32, (8, 128), 0)
        spread = jnp.where(lane // 16 == row_at, spread, 0.0)
        rows.append(jnp.sum(spread, axis=0, keepdims=True))
    total = energies[:1]
    rows = jnp.concatenate((*rows, total, total), axis=0)
    message[...] = jnp.broadcast_to(rows[None], (32, 4, 128))


def finish(returned, orbitals, energies):
    vmem = pl.BlockSpec(memory_space=pltpu.VMEM)
    return pl.pallas_call(
        finish_kernel,
        out_shape=(
            jax.ShapeDtypeStruct((32, 8, 128), f32),
            jax.ShapeDtypeStruct((32, 4, 128), f32),
        ),
        in_specs=[vmem] * 3,
        out_specs=(vmem, vmem),
        compiler_params=pltpu.CompilerParams(vmem_limit_bytes=8 * MIB),
        name="finish",
    )(returned, orbitals, energies)


def close_kernel(messages, matrix, energy):
    total = jnp.sum(messages[...], axis=0)
    lane = lax.broadcasted_iota(jnp.int32, (32, 128), 1)
    row = lax.broadcasted_iota(jnp.int32, (32, 128), 0)
    spread = jnp.concatenate(
        [jnp.broadcast_to(total[k : k + 1], (16, 128)) for k in range(2)], axis=0
    )
    spread = jnp.where(lane // 8 == row % 8 * 2 + row // 8 % 2, spread, 0.0)
    gather = jnp.where(
        lax.broadcasted_iota(jnp.int32, (128, 128), 0) % 8
        == lax.broadcasted_iota(jnp.int32, (128, 128), 1),
        1.0,
        0.0,
    )
    spread = jnp.dot(spread, gather, precision=highest, preferred_element_type=f32)
    for k in range(2):
        for part in range(2):
            first = k * 16 + part * 8
            matrix[k, part] = spread[first : first + 8, :8]
    energy[...] = total[2:3, :1]


def close(messages):
    vmem = pl.BlockSpec(memory_space=pltpu.VMEM)
    return pl.pallas_call(
        close_kernel,
        out_shape=(jax.ShapeDtypeStruct((2, 2, 8, 8), f32), jax.ShapeDtypeStruct((1, 1), f32)),
        in_specs=[vmem],
        out_specs=(vmem, vmem),
        compiler_params=pltpu.CompilerParams(vmem_limit_bytes=4 * MIB),
        name="close",
    )(messages)


def on_device(orbitals, band_counts, pair_slot, kernel):
    left, right, twiddle = (jnp.asarray(table) for table in constants())
    groups = lax.axis_size("ka")
    scale = -1.0 / (16.0 * 32768.0)

    before = lax.ppermute(orbitals, "ka", [(i, (i + 1) % groups) for i in range(groups)])
    chosen = choose(pair_slot, kernel.reshape(16, 8, 128))
    counts = band_counts.reshape(1, 16)
    orbitals = orbitals.reshape(16, 16, 128)
    packed = pack(orbitals, before.reshape(16, 16, 128), chosen)
    received = lax.all_to_all(packed, "ga", 0, 0, tiled=True)

    def shown(value, bit):
        return lax.ppermute(value, "ga", [(i, i ^ bit) for i in range(32)])

    tables = (left, right, twiddle)
    next_core = shown(received[:, :40], 1)
    next_y, next_z = shown(received[:, BAND_ROWS[0]], 16), shown(received[:, BAND_ROWS[1]], 2)
    total, screen = exchange(scale, 0, counts, received, (next_core,), tables)
    (total,) = exchange(scale, 1, counts, received, (next_core,), tables, screen, total)
    next_y, next_z, total = lax.optimization_barrier((next_y, next_z, total))
    far = (shown(next_y, 1), shown(next_z, 1))
    (total,) = exchange(scale, 2, counts, received, (next_y, next_z), tables, screen, total)
    leaving, energy = exchange(scale, 3, counts, received, far, tables, screen, total)

    def shown_energy(value, bit):
        return lax.ppermute(value, "ka", [(i, i ^ bit) for i in range(groups)])

    first = shown_energy(energy, 1)
    returned = lax.all_to_all(leaving, "ga", 0, 0, tiled=True)
    energy = energy + first
    energy = energy + shown_energy(energy, 2)
    energy = energy + shown_energy(energy, 4)
    vectors, message = finish(returned.reshape(2, 4, 2, 2, 48, 128), orbitals, energy)
    matrix, energy = close(lax.all_to_all(message, "ga", 0, 0, tiled=True))
    return (vectors.reshape(2, 8, 2, 1, 1024), matrix, energy[0, 0])


def solution(mesh):
    in_specs = (P("ka", None, None, "ga", None), P(), P(), P(None, None, "ga"))
    out_specs = (P("ka", None, None, "ga", None), P("ka", None, None, None), P())
    return jax.shard_map(
        on_device, mesh=mesh, in_specs=in_specs, out_specs=out_specs, check_vma=False
    )
```

```python
import functools

import numpy as np
import jax
import jax.numpy as jnp
from jax import lax
from jax.experimental import pallas as pl
from jax.experimental.pallas import tpu as pltpu
from jax.sharding import PartitionSpec as P


highest = lax.Precision.HIGHEST
f32 = jnp.float32
bf16 = jnp.bfloat16


def embed(matrix):
    return np.block([[matrix.real, -matrix.imag], [matrix.imag, matrix.real]])


def split(matrix):
    high = matrix.astype(np.float32).astype(bf16)
    low = (matrix - high.astype(np.float64)).astype(np.float32).astype(bf16)
    return high, low


def constants():
    rows = np.arange(128)
    x_at, yh_at = rows // 8, rows % 8
    jj_at, glo_at, gxh_at = rows // 64, rows // 8 % 8, rows % 8
    forward, inverse = [], []
    for parity in range(2):
        gx_at = 4 * gxh_at + 2 * jj_at + parity
        phase = gx_at[:, None] * x_at[None, :] / 32.0 + glo_at[:, None] * yh_at[None, :] / 8.0
        real = embed(np.exp(-2j * np.pi * phase))
        for held, matrix in ((forward, real), (inverse, real.T)):
            high, low = split(matrix)
            held.append(np.concatenate((high, low), axis=1))
    lanes = np.arange(128)
    first, last = lanes // 32, lanes % 32
    phase = first[:, None] * first[None, :] / 4.0 + last[:, None] * last[None, :] / 32.0
    real = embed(np.exp(-2j * np.pi * phase)).T
    right = []
    for matrix in (real, real.T):
        high, low = split(matrix)
        right.append(np.concatenate((high, low), axis=0))
    turn = 2.0 * np.pi * (glo_at[:, None] * first[None, :]) / 32.0
    twiddle = np.stack((np.cos(turn), np.sin(turn))).astype(np.float32)
    return np.stack(forward + inverse), np.stack(right), twiddle


def two_terms(value):
    high = value.astype(bf16)
    low = (value - high.astype(f32)).astype(bf16)
    return high, low


MIB = 1 << 20


def place():
    member = lax.axis_index("ga")
    return lax.axis_index("ka"), member // 16, member // 4 % 4, member // 2 % 2, member % 2


def y_band(y_at, core):
    return 4 * y_at + core


def z_band(y_at, k, core):
    return 2 + 4 * ((y_at + k) % 2) + core


def choose_kernel(pair_slot, kernel, chosen):
    group = lax.axis_index("ka")
    partner_group = lax.rem(group + 7, 8)
    for k2 in range(4):
        second = (group if k2 < 2 else partner_group) * 2 + k2 % 2
        for k in range(2):
            block = kernel[pair_slot[group * 2 + k, second]]
            high, low = two_terms(block)
            for core in range(2):
                rows = slice(core * 4, core * 4 + 4)
                chosen[k2 * 2 + k, core] = jnp.concatenate((high[rows], low[rows]), axis=0)


def choose(pair_slot, kernel):
    vmem = pl.BlockSpec(memory_space=pltpu.VMEM)
    return pl.pallas_call(
        choose_kernel,
        out_shape=jax.ShapeDtypeStruct((8, 2, 8, 128), bf16),
        in_specs=[pl.BlockSpec(memory_space=pltpu.SMEM), vmem],
        out_specs=vmem,
        compiler_params=pltpu.CompilerParams(vmem_limit_bytes=4 * MIB),
        name="choose",
    )(pair_slot, kernel)


KERNEL_ROWS = slice(0, 8)
BAND_ROWS = (slice(8, 24), slice(24, 40))
OWN_ROWS = (slice(40, 56), slice(56, 72))


def pack_kernel(orbitals, before, chosen, packed):
    for k2 in range(4):
        source = orbitals if k2 < 2 else before
        for k in range(2):
            for quarter in range(4):
                y_at, core = quarter // 2, quarter % 2
                to = y_at * 16 + k2 * 4 + k * 2 + core
                packed[to, KERNEL_ROWS] = chosen[k2 * 2 + k, core]
                packed[to, BAND_ROWS[0]] = source[k2 % 2 * 8 + y_band(y_at, core)]
                packed[to, BAND_ROWS[1]] = source[k2 % 2 * 8 + z_band(y_at, k, core)]
                for j in range(2):
                    packed[to, OWN_ROWS[j]] = orbitals[k * 8 + quarter * 2 + j]


def pack(orbitals, before, chosen):
    vmem = pl.BlockSpec(memory_space=pltpu.VMEM)
    return pl.pallas_call(
        pack_kernel,
        out_shape=jax.ShapeDtypeStruct((32, 72, 128), bf16),
        in_specs=[vmem, vmem, vmem],
        out_specs=vmem,
        compiler_params=pltpu.CompilerParams(vmem_limit_bytes=4 * MIB),
        name="pack",
    )(orbitals, before, chosen)


def screen_of(received, other, core, scale, screen):
    halves = []
    for half in (received, other):
        half = half[:, KERNEL_ROWS].astype(f32)
        halves.append(((half + pltpu.roll(half, 4, 1)) * scale).reshape(256, 128))
    row = lax.broadcasted_iota(jnp.int32, (256, 128), 0) % 8
    raw = jnp.where(row // 4 == core, halves[0], halves[1]).reshape(4, 64, 128)
    lane_group = lax.broadcasted_iota(jnp.int32, (64, 128), 1) // 32
    for j in range(4):
        placed = jnp.zeros((64, 128), f32)
        for i in range(4):
            shift = (i - j) % 4 * 32
            moved = pltpu.roll(raw[i], shift, 1) if shift else raw[i]
            placed = jnp.where(lane_group == i, moved, placed)
        screen[j % 2, (j // 2) * 64 : (j // 2) * 64 + 64] = placed


def thrice(table, axis):
    size = table.shape[axis] // 2
    return jnp.concatenate((table, lax.slice_in_dim(table, 0, size, axis=axis)), axis=axis)


def enter(parts, table):
    stacked = jnp.concatenate([jnp.concatenate(parts[part], axis=1) for part in range(2)], axis=0)
    high, low = two_terms(stacked)
    return jnp.dot(
        thrice(table, 1), jnp.concatenate((high, high, low), axis=0), preferred_element_type=f32
    )


def across(turned, table, cosine, sine):
    lines = []
    for a in range(2):
        real = turned[:128, a * 128 : a * 128 + 128]
        imag = turned[128:, a * 128 : a * 128 + 128]
        lines.append(
            jnp.concatenate((real * cosine + imag * sine, imag * cosine - real * sine), axis=1)
        )
    high, low = two_terms(jnp.concatenate(lines, axis=0))
    return jnp.dot(
        jnp.concatenate((high, high, low), axis=1), thrice(table, 0), preferred_element_type=f32
    )


def screened(spectra, factor, table):
    factor = jnp.concatenate((factor, factor), axis=1)
    factor = jnp.concatenate((factor, factor), axis=0)
    high, low = two_terms(spectra * factor)
    return jnp.dot(
        jnp.concatenate((high, high, low), axis=1), thrice(table, 0), preferred_element_type=f32
    )


def leave(lines, table, cosine, sine):
    reals, imags = [], []
    for a in range(2):
        real = lines[a * 128 : a * 128 + 128, :128]
        imag = lines[a * 128 : a * 128 + 128, 128:]
        reals.append(real * cosine - imag * sine)
        imags.append(imag * cosine + real * sine)
    stacked = jnp.concatenate(
        (jnp.concatenate(reals, axis=1), jnp.concatenate(imags, axis=1)), axis=0
    )
    high, low = two_terms(stacked)
    return jnp.dot(
        thrice(table, 1), jnp.concatenate((high, high, low), axis=0), preferred_element_type=f32
    )


LEVELS = 10
BASE = 2 * LEVELS + 1


def remainder(value):
    high = value.astype(bf16)
    wide = high.astype(f32)
    share = (value - wide) / jnp.where(wide == 0.0, 1.0, wide)
    return high, jnp.floor(share * (256.0 * LEVELS) + 0.5)


def coded(real, imag):
    real, first = remainder(real)
    imag, second = remainder(imag)
    return jnp.concatenate((real, imag), axis=1), first * BASE + second


def decoded(high, code):
    first = jnp.floor(code * (1.0 / BASE) + 0.5)
    second = code - first * BASE
    step = 1.0 / (256.0 * LEVELS)
    return high[..., :8, :] * (1.0 + first * step), high[..., 8:, :] * (1.0 + second * step)


def exchange_kernel(scale, call, counts, received, *refs):
    left, right, twiddle, *rest = refs[SOURCES[call] :]
    group, y_at, k2, k, core = place()
    if call < 2:
        source = refs[0] if call else received
        partners = [lambda rows, at=at: source[rows, at] for at in BAND_ROWS]
    else:
        partners = [lambda rows, ref=ref: ref[rows] for ref in refs[:2]]
    if call == 0:
        total, screen = rest
        screen_of(received, refs[0], core, scale, screen)
        held = None
    else:
        screen, held, total = rest[:3]
        if call == 3:
            left_memory, energy, total, leaving, sent = rest[2:]
    k2_at = lax.rem(group + 8 - k2 // 2, 8) * 2 + k2 % 2
    core_from = 1 - core if call % 2 else core
    bands = (
        y_band(1 - y_at if call >= 2 else y_at, core_from),
        z_band(y_at, 1 - k if call >= 2 else k, core_from),
    )
    lane = lax.broadcasted_iota(jnp.int32, (1, 16), 1)

    def count_of(kpoint):
        return jnp.sum(jnp.where(lane == kpoint, counts[...].astype(f32), 0.0), axis=1, keepdims=True)

    count = count_of(k2_at)
    kept = [
        jnp.where(count > band.astype(f32), 1.0, 0.0).reshape(1, 1, 1) for band in bands
    ]
    others, chains = [], []
    for half in range(2):
        other = partners[half](slice(0, 32)).astype(f32)
        other_real, other_imag = other[:, :8], other[:, 8:]
        sums, gaps = [[], []], [[], []]
        for a in range(2):
            own = received[:, OWN_ROWS[a]].astype(f32)
            own_real, own_imag = own[:, :8], own[:, 8:]
            density = (
                own_real * other_real + own_imag * other_imag,
                own_imag * other_real - own_real * other_imag,
            )
            for part in range(2):
                low, high = density[part][:16], density[part][16:]
                sums[part].append((low + high).reshape(128, 128))
                gaps[part].append((low - high).reshape(128, 128))
        others.append((half, kept[half]))
        chains += [(0, sums), (1, gaps)]
    cosine, sine = twiddle[0], twiddle[1]
    values = [enter(parts, left[parity]) for parity, parts in chains]
    values = [across(value, right[0], cosine, sine) for value in values]
    values = [
        screened(value, screen[parity], right[1])
        for value, (parity, parts) in zip(values, chains)
    ]
    values = [
        leave(value, left[2 + parity], cosine, sine)
        for value, (parity, parts) in zip(values, chains)
    ]
    backs = [values[2 * half : 2 * half + 2] for half in range(2)]
    for side in range(2):
        rows = slice(side * 16, side * 16 + 16)
        codes = []
        for a in range(2):
            add_real, add_imag = 0.0, 0.0
            if held is not None:
                add_real, add_imag = held[rows, 2 * a], held[rows, 2 * a + 1]
            for (even, odd), (half, factor) in zip(backs, others):
                field = even + odd if side == 0 else even - odd
                other = partners[half](rows).astype(f32) * factor
                b_real, b_imag = other[:, :8], other[:, 8:]
                real = field[:128, a * 128 : a * 128 + 128].reshape(16, 8, 128)
                imag = field[128:, a * 128 : a * 128 + 128].reshape(16, 8, 128)
                add_real += b_real * real - b_imag * imag
                add_imag += b_real * imag + b_imag * real
            total[rows, 2 * a] = add_real
            total[rows, 2 * a + 1] = add_imag
            if call == 3:
                leaving[rows, 16 * a : 16 * a + 16], code = coded(add_real, add_imag)
                codes.append(code)
        if call == 3:
            leaving[rows, 32:48] = jnp.concatenate(codes, axis=1).astype(bf16)

    if call == 3:
        copy = pltpu.make_async_copy(leaving, left_memory, sent)
        copy.start()
        count = count_of(group * 2 + k)
        energy_sum = jnp.zeros((8, 128), f32)
        for a in range(2):
            occupied = jnp.where(count > (y_at * 4 + core * 2 + a).astype(f32), 1.0, 0.0)
            own = received[:, OWN_ROWS[a]].astype(f32)
            both = own[:, :8] * total[:, 2 * a] + own[:, 8:] * total[:, 2 * a + 1]
            energy_sum += jnp.sum(both, axis=0) * occupied
        energy[...] = jnp.full((8, 128), jnp.sum(energy_sum) * (1.0 / (32.0 * 32768.0)), f32)
        copy.wait()


SOURCES = (1, 1, 2, 2)


def exchange(scale, call, counts, received, partners, tables, *carried):
    vmem = pl.BlockSpec(memory_space=pltpu.VMEM)
    operands = (counts, received, *partners, *tables, *carried)
    shapes, scratch = [jax.ShapeDtypeStruct((32, 4, 8, 128), f32)], []
    if call == 3:
        shapes = [jax.ShapeDtypeStruct((32, 48, 128), bf16), jax.ShapeDtypeStruct((8, 128), f32)]
        scratch = [
            pltpu.VMEM((32, 4, 8, 128), f32),
            pltpu.VMEM((32, 48, 128), bf16),
            pltpu.SemaphoreType.DMA(()),
        ]
    if call == 0:
        shapes.append(jax.ShapeDtypeStruct((2, 128, 128), f32))
    return pl.pallas_call(
        functools.partial(exchange_kernel, scale, call),
        out_shape=tuple(shapes),
        in_specs=[vmem] * len(operands),
        out_specs=(pl.BlockSpec(memory_space=pl.ANY) if call == 3 else vmem, *(vmem,) * (len(shapes) - 1)),
        scratch_shapes=scratch,
        compiler_params=pltpu.CompilerParams(vmem_limit_bytes=24 * MIB),
        cost_estimate=pl.CostEstimate(
            flops=2 * 12 * 2 * 512 * 256 * 256, bytes_accessed=4 << 20, transcendentals=0
        ),
    )(*operands)


def finish_kernel(returned, orbitals, energies, vectors, message):
    fields = []
    for k in range(2):
        for y_at in range(2):
            for core in range(2):
                sums = [0.0] * 4
                for k2 in range(4):
                    block = returned[y_at, k2, k, core].astype(f32)
                    for a in range(2):
                        parts = decoded(
                            block[16 * a : 16 * a + 16], block[32 + 8 * a : 40 + 8 * a]
                        )
                        for part in range(2):
                            sums[2 * a + part] += parts[part]
                fields += [value.reshape(1, 8, 128) for value in sums]
    fields = jnp.concatenate(fields, axis=0)
    vectors[...] = fields
    lane = lax.broadcasted_iota(jnp.int32, (8, 128), 1)
    rows = []
    for k in range(2):
        left = jnp.concatenate(
            [orbitals[k * 8 : k * 8 + 8, row] for row in range(16)], axis=1
        ).astype(f32)
        own = fields[k * 16 : k * 16 + 16].reshape(8, 2, 8, 128)
        real = [own[:, 0, row] for row in range(8)]
        imag = [own[:, 1, row] for row in range(8)]
        right = jnp.concatenate(
            (
                jnp.concatenate(real + imag, axis=1),
                jnp.concatenate(imag + [-value for value in real], axis=1),
            ),
            axis=0,
        )
        left = left.astype(bf16)
        product = jnp.zeros((8, 16), f32)
        for _ in range(3):
            term = right.astype(bf16)
            right = right - term.astype(f32)
            product += lax.dot_general(
                left, term, (((1,), (1,)), ((), ())), preferred_element_type=f32
            )
        spread = jnp.concatenate([product * (1.0 / 32768.0)] * 8, axis=1)
        row_at = lax.broadcasted_iota(jnp.int32, (8, 128), 0)
        spread = jnp.where(lane // 16 == row_at, spread, 0.0)
        rows.append(jnp.sum(spread, axis=0, keepdims=True))
    total = energies[:1]
    rows = jnp.concatenate((*rows, total, total), axis=0)
    message[...] = jnp.broadcast_to(rows[None], (32, 4, 128))


def finish(returned, orbitals, energies):
    vmem = pl.BlockSpec(memory_space=pltpu.VMEM)
    return pl.pallas_call(
        finish_kernel,
        out_shape=(
            jax.ShapeDtypeStruct((32, 8, 128), f32),
            jax.ShapeDtypeStruct((32, 4, 128), f32),
        ),
        in_specs=[vmem] * 3,
        out_specs=(vmem, vmem),
        compiler_params=pltpu.CompilerParams(vmem_limit_bytes=8 * MIB),
        name="finish",
    )(returned, orbitals, energies)


def close_kernel(messages, matrix, energy):
    total = jnp.sum(messages[...], axis=0)
    lane = lax.broadcasted_iota(jnp.int32, (32, 128), 1)
    row = lax.broadcasted_iota(jnp.int32, (32, 128), 0)
    spread = jnp.concatenate(
        [jnp.broadcast_to(total[k : k + 1], (16, 128)) for k in range(2)], axis=0
    )
    spread = jnp.where(lane // 8 == row % 8 * 2 + row // 8 % 2, spread, 0.0)
    gather = jnp.where(
        lax.broadcasted_iota(jnp.int32, (128, 128), 0) % 8
        == lax.broadcasted_iota(jnp.int32, (128, 128), 1),
        1.0,
        0.0,
    )
    spread = jnp.dot(spread, gather, precision=highest, preferred_element_type=f32)
    for k in range(2):
        for part in range(2):
            first = k * 16 + part * 8
            matrix[k, part] = spread[first : first + 8, :8]
    energy[...] = total[2:3, :1]


def close(messages):
    vmem = pl.BlockSpec(memory_space=pltpu.VMEM)
    return pl.pallas_call(
        close_kernel,
        out_shape=(jax.ShapeDtypeStruct((2, 2, 8, 8), f32), jax.ShapeDtypeStruct((1, 1), f32)),
        in_specs=[vmem],
        out_specs=(vmem, vmem),
        compiler_params=pltpu.CompilerParams(vmem_limit_bytes=4 * MIB),
        name="close",
    )(messages)


def on_device(orbitals, band_counts, pair_slot, kernel):
    left, right, twiddle = (jnp.asarray(table) for table in constants())
    groups = lax.axis_size("ka")
    scale = -1.0 / (16.0 * 32768.0)

    before = lax.ppermute(orbitals, "ka", [(i, (i + 1) % groups) for i in range(groups)])
    chosen = choose(pair_slot, kernel.reshape(16, 8, 128))
    counts = band_counts.reshape(1, 16)
    orbitals = orbitals.reshape(16, 16, 128)
    packed = pack(orbitals, before.reshape(16, 16, 128), chosen)
    received = lax.all_to_all(packed, "ga", 0, 0, tiled=True)

    def shown(value, bit):
        return lax.ppermute(value, "ga", [(i, i ^ bit) for i in range(32)])

    tables = (left, right, twiddle)
    next_core = shown(received[:, :40], 1)
    next_y, next_z = shown(received[:, BAND_ROWS[0]], 16), shown(received[:, BAND_ROWS[1]], 2)
    total, screen = exchange(scale, 0, counts, received, (next_core,), tables)
    (total,) = exchange(scale, 1, counts, received, (next_core,), tables, screen, total)
    next_y, next_z, total = lax.optimization_barrier((next_y, next_z, total))
    far = (shown(next_y, 1), shown(next_z, 1))
    (total,) = exchange(scale, 2, counts, received, (next_y, next_z), tables, screen, total)
    leaving, energy = exchange(scale, 3, counts, received, far, tables, screen, total)

    def shown_energy(value, bit):
        return lax.ppermute(value, "ka", [(i, i ^ bit) for i in range(groups)])

    first = shown_energy(energy, 1)
    returned = lax.all_to_all(leaving, "ga", 0, 0, tiled=True)
    energy = energy + first
    energy = energy + shown_energy(energy, 2)
    energy = energy + shown_energy(energy, 4)
    vectors, message = finish(returned.reshape(2, 4, 2, 2, 48, 128), orbitals, energy)
    matrix, energy = close(lax.all_to_all(message, "ga", 0, 0, tiled=True))
    return (vectors.reshape(2, 8, 2, 1, 1024), matrix, energy[0, 0])


def solution(mesh):
    in_specs = (P("ka", None, None, "ga", None), P(), P(), P(None, None, "ga"))
    out_specs = (P("ka", None, None, "ga", None), P("ka", None, None, None), P())
    return jax.shard_map(
        on_device, mesh=mesh, in_specs=in_specs, out_specs=out_specs, check_vma=False
    )
```
